32 devices in a mesh: rep: 2 (over z, core), dp: 16 (over x, y).
Axes of the slice: x: 4, y: 4, z: 1, core: 2. Of those that a mesh axis runs over, the one named last changes fastest.
The devices are a block of a 4x4x8 slice.
Arguments:
- x: bfloat16 [32, 4096, 896], P(('rep', 'dp')), parts along dimension 0
- dy: bfloat16 [32, 4096, 896], P(('rep', 'dp')), parts along dimension 0
- w_gate: bfloat16 [2, 896, 2304], P(None, 'dp')
- w_up: bfloat16 [2, 896, 2304], P(None, 'dp')
- w_down: bfloat16 [2, 2304, 896], P(None, 'dp')
- m_w_gate: float32 [2, 896, 2304], P(None, 'dp')
- m_w_up: float32 [2, 896, 2304], P(None, 'dp')
- m_w_down: float32 [2, 2304, 896], P(None, 'dp')
- v_w_gate: float32 [2, 896, 2304], P(None, 'dp')
- v_w_up: float32 [2, 896, 2304], P(None, 'dp')
- v_w_down: float32 [2, 2304, 896], P(None, 'dp')
Outputs:
- output 1: bfloat16 [4, 896, 2304], P('rep', 'dp'), parts along dimension 0
- output 2: bfloat16 [4, 896, 2304], P('rep', 'dp'), parts along dimension 0
- output 3: bfloat16 [4, 2304, 896], P('rep', 'dp'), parts along dimension 0
- output 4: float32 [4, 896, 2304], P('rep', 'dp'), parts along dimension 0
- output 5: float32 [4, 896, 2304], P('rep', 'dp'), parts along dimension 0
- output 6: float32 [4, 2304, 896], P('rep', 'dp'), parts along dimension 0
- output 7: float32 [4, 896, 2304], P('rep', 'dp'), parts along dimension 0
- output 8: float32 [4, 896, 2304], P('rep', 'dp'), parts along dimension 0
- output 9: float32 [4, 2304, 896], P('rep', 'dp'), parts along dimension 0
There are 2 independent parts. The reference program is written for one: setup_inputs(seed, part) draws one part's arguments, and reference() takes and returns one part's arrays. A program takes and returns all parts, laid end to end along the dimension named above; an argument that names none is the same for every part.
All inputs are finite; a program needn't handle non-finite values.
Results may differ from the reference program's by a relative error of at most 0.022.
Values are sent between devices in bfloat16 or wider.
A program may use at most 768 MiB of HBM per device.

```python
import jax
import jax.numpy as jnp
from jax import lax

SEQUENCES = 16
TOKENS = 4096
D = 896
FF = 2304
LAYERS = 2
NAMES = ("w_gate", "w_up", "w_down")
SHAPES = {"w_gate": (LAYERS, D, FF), "w_up": (LAYERS, D, FF), "w_down": (LAYERS, FF, D)}


def bump(key, n, height):
    away = (jnp.arange(n, dtype=jnp.int32) - jax.random.randint(key, (), 0, n, jnp.int32)) % n
    return jnp.where(away < n // 8, height, 1.0)


def together(key, own, strength):
    shared = jax.random.normal(key, own.shape[1:], jnp.float32)
    return (own + strength * shared) * lax.rsqrt(1 + strength * strength)


def setup_inputs(seed: int = 0, part: int = 0) -> dict:
    kx, kdy, ka, kb, kz, kf, kh, kl, *keys = jax.random.split(jax.random.key(seed), 8 + 3 * len(NAMES))
    kx, kdy, ka, kb = (jax.random.fold_in(k, part) for k in (kx, kdy, ka, kb))
    kw, km, kv = (keys[i::3] for i in range(3))
    shape = (SEQUENCES, TOKENS, D)
    much_x, much_dy = jax.random.uniform(kz, (2,), jnp.float32, 0.0, 1.0)
    loud = 2.0 ** jax.random.uniform(jax.random.fold_in(kz, 1), (), jnp.float32, -1.0, 2.0)
    layers = 2.0 ** jax.random.uniform(kl, (LAYERS, 1, 1), jnp.float32, -1.0, 1.0)
    x = together(ka, jax.random.normal(kx, shape, jnp.float32), much_x) * bump(kf, D, 4.0)
    dy = together(kb, jax.random.normal(kdy, shape, jnp.float32), much_dy)
    drawn = {"x": x.astype(jnp.bfloat16), "dy": (loud * dy * (SEQUENCES * TOKENS) ** -0.5).astype(jnp.bfloat16)}
    for key, name in zip(kw, NAMES, strict=True):
        w = jax.random.normal(key, SHAPES[name], jnp.float32) * SHAPES[name][1] ** -0.5
        drawn[name] = (w * {"w_gate": 1.0, "w_up": bump(kh, FF, 4.0), "w_down": layers}[name]).astype(jnp.bfloat16)
    for key, name in zip(km, NAMES, strict=True):
        drawn[f"m_{name}"] = 0.1 * jax.random.normal(key, SHAPES[name], jnp.float32)
    for key, name in zip(kv, NAMES, strict=True):
        drawn[f"v_{name}"] = jax.random.uniform(key, SHAPES[name], jnp.float32, 0.005, 0.015)
    return drawn


def matmul(a, w):
    return jnp.dot(a, w, preferred_element_type=jnp.float32).astype(jnp.bfloat16)


def normed(h):
    wide = h.astype(jnp.float32)
    scale = lax.rsqrt(jnp.mean(wide**2, -1, keepdims=True) + 1e-6)
    return (wide * scale).astype(jnp.bfloat16)


def layer(h, w):
    a = normed(h)
    gate = jnp.dot(a, w["w_gate"], preferred_element_type=jnp.float32)
    up = jnp.dot(a, w["w_up"], preferred_element_type=jnp.float32)
    return h + matmul((jax.nn.silu(gate) * up).astype(jnp.bfloat16), w["w_down"])


def adamw(w, m, v, g):
    m = 0.9 * m + 0.1 * g
    v = 0.95 * v + 0.05 * g * g
    step = m * lax.rsqrt(v + 1e-8) + 0.1 * w
    return (w - 0.02 * step).astype(jnp.bfloat16), m, v


def clipped(gradients, sum_of_squares, count):
    factor = jnp.minimum(1.0, 0.5 * lax.rsqrt(sum_of_squares / count + 1e-30))
    return [g * factor for g in gradients]


def stack(weights, h):
    return lax.scan(lambda h, w: (layer(h, w), None), h, weights)[0]


def reference(x, dy, w_gate, w_up, w_down, m_w_gate, m_w_up, m_w_down, v_w_gate, v_w_up, v_w_down):
    weights = dict(zip(NAMES, (w_gate, w_up, w_down), strict=True))

    def take(so_far, sequence):
        h, by_y = sequence
        _, back = jax.vjp(lambda w: stack(w, h), weights)
        return jax.tree.map(lambda total, term: total + term.astype(jnp.float32), so_far, back(by_y)[0]), None

    none_yet = {name: jnp.zeros(w.shape, jnp.float32) for name, w in weights.items()}
    by_weights, _ = lax.scan(take, none_yet, (x, dy))
    gradients = [by_weights[name].astype(jnp.bfloat16).astype(jnp.float32) for name in NAMES]
    gradients = clipped(gradients, sum(jnp.sum(g * g) for g in gradients), sum(g.size for g in gradients))
    new = [
        adamw(w.astype(jnp.float32), m, v, g)
        for w, m, v, g in zip((w_gate, w_up, w_down), (m_w_gate, m_w_up, m_w_down), (v_w_gate, v_w_up, v_w_down), gradients, strict=True)
    ]
    return tuple(one[which] for which in range(3) for one in new)
```

```python
import math

import jax
import jax.numpy as jnp
from jax import lax
from jax.experimental import pallas as pl
from jax.experimental.pallas import tpu as pltpu
from jax.sharding import PartitionSpec as P

bf16, f32 = jnp.bfloat16, jnp.float32
MESH = pl.DeviceIdType.MESH
CH = 256
TB = 2048
TD = 2 * CH
TILE = SUB, LANES = 8, 128
PACK = 2 * SUB
WIDE = 2 * CH
VMEM_BYTES = 67043328
AHEAD = 4
SLOTS = HALVES = KINDS = PAIR = 2
NN = (((1,), (0,)), ((), ()))
NT = (((1,), (1,)), ((), ()))
TN = (((0,), (0,)), ((), ()))


def dot(a, b, dims=NN):
    return lax.dot_general(a, b, dims, preferred_element_type=f32)


def adamw_kernel(count, squares, *refs):
    groups = len(refs) // 11
    arrays, out, held, sems = refs[: groups * 4], refs[groups * 4 : groups * 7], refs[groups * 7 : -1], refs[-1]
    for i, (array, here) in enumerate(zip(arrays, held, strict=True)):
        pltpu.make_async_copy(array, here, sems.at[i]).start()
    total = jnp.sum(squares[...], keepdims=True)
    factor = jnp.minimum(1.0, 0.5 * lax.rsqrt(total / count + 1e-30))
    stores = []
    for group in range(groups):
        g_ref, w_ref, m_ref, v_ref = held[group * 4 : group * 4 + 4]
        for i in range(group * 4, group * 4 + 4):
            pltpu.make_async_copy(arrays[i], held[i], sems.at[i]).wait()
        def one_layer(at, _):
            g = g_ref[at].astype(f32) * factor
            w = w_ref[at].astype(f32)
            m = 0.9 * m_ref[at] + 0.1 * g
            v = 0.95 * v_ref[at] + 0.05 * g * g
            step = m * lax.rsqrt(v + 1e-8) + 0.1 * w
            w_ref[at] = (w - 0.02 * step).astype(bf16)
            m_ref[at] = m
            v_ref[at] = v
            return 0

        lax.fori_loop(0, g_ref.shape[0], one_layer, 0)
        for i, here in enumerate((w_ref, m_ref, v_ref)):
            stores.append(pltpu.make_async_copy(here, out[group * 3 + i], sems.at[group * 4 + i]))
            stores[-1].start()
    for copy in stores:
        copy.wait()


def step_kernel(n, x, dy, wg, wu, wd, *refs):
    (gg_h, gu_h, gd_h, ss, wgu_h, wd_h, st_h, hid_h, a0_h, h1_h, rA) = refs[:11]
    (gg, gu, gd, act, stage, wcomb, wdc, scl, acc, sst, ssr, lb, l2) = refs[11:24]
    (sx, sw, swd, s_stage, shid, sm, ag_loc, ag_s, ag_r, rs_s, rs_r, rs_l, ss_s, ss_r) = refs[24:]
    L, R, FF = wg.shape
    RF, D = wd.shape[1:]
    T = x.shape[0]
    S = math.isqrt(n)
    NC = FF // CH
    NI = L * NC
    NJ = T // TB
    NB = T // TD
    NW = 3
    HW = RF // 2 // NW
    RC = RF // NC
    RB = R + SUB * pl.cdiv(D, CH)
    me, rep = lax.axis_index("dp"), lax.axis_index("rep")
    px, py = me // S, me % S
    par = rep % SLOTS
    one_chunk = wgu_h.at[0, 0, 0]
    partner = {"rep": rep + 1 - 2 * par, "dp": me}
    aT, dyT = act.at[0], act.at[1]
    vmem = pltpu.VMEM

    def at(ix, iy):
        return {"dp": (ix % S) * S + iy % S}

    def send(src, dst, s, r, to):
        pltpu.make_async_remote_copy(src_ref=src, dst_ref=dst, send_sem=s, recv_sem=r, device_id=to, device_id_type=MESH).start()

    def wait(ref, sem):
        pltpu.make_async_copy(ref, ref, sem).wait()

    def cols(c):
        return pl.ds(pl.multiple_of(c * CH, CH), CH)

    def blocks(b, size):
        return pl.ds(pl.multiple_of(b * size, size), size)

    def load_w(i, slot):
        for h in range(HALVES):
            pltpu.make_async_copy(wgu_h.at[h, i // NC, i % NC], wcomb.at[slot, :, :, :, pl.ds(h * CH, CH)], sw.at[slot, h]).start()

    def wait_w(slot):
        for h in range(HALVES):
            wait(one_chunk, sw.at[slot, h])

    def load_wd(l, c, slot):
        return pltpu.make_async_copy(wd_h.at[l, cols(c)], wdc.at[slot], swd.at[slot])

    def item(k):
        return L - 1 - k // NC, k % NC

    def load_stage(k, j):
        l, c = item(k)
        return pltpu.make_async_copy(st_h.at[l, c, :, blocks(j, TB)], stage.at[j], s_stage.at[j])

    def norm(src, dst):
        def rows(g):
            return pl.ds(g * PACK, PACK)

        total = jnp.zeros((SUB, src.shape[1]), f32)
        for g in range(D // (PACK)):
            wide = src[rows(g), :].astype(f32)
            wide = wide * wide
            total += wide[:SUB] + wide[SUB:]
        scale = lax.rsqrt(jnp.sum(total, axis=0, keepdims=True) / D + 1e-6)
        for g in range(D // (PACK)):
            dst[rows(g), :] = (src[rows(g), :].astype(f32) * scale).astype(bf16)
        return scale

    def forward(hiddenT, w_down, xs, dys, h1s, wl, wdl, sh, sdy):
        def with_down(i):
            return pl.when((i % NC >= NW) & (i % NC % PAIR == 1))

        def rows(d, c):
            return pl.ds(pl.multiple_of(d * RF + par * (RF // 2) + (c - NW) // PAIR * HW, 8), HW)

        def ag1(i):
            l, c = i // NC, i % NC
            p = i % AHEAD
            src, own = wl.at[par, l, :, cols(c)], wgu_h.at[par, l, c, px, py]
            for r in range(1, S):
                send(src, own, ag_s.at[0, p, 0], ag_r.at[0, i, 0], at(px + r * (1 - par), py + r * par))
            pltpu.make_async_copy(src, own, ag_loc.at[p, 0]).start()

            @with_down(i)
            def _():
                src, own = wdl.at[l, par * NW + (c - NW) // PAIR], wd_h.at[l, rows(me, c)]
                for r in range(1, S):
                    send(src, own, ag_s.at[0, p, 1], ag_r.at[0, i, 1], at(px + r * (1 - par), py + r * par))
                pltpu.make_async_copy(src, own, ag_loc.at[p, 1]).start()

        def ag2(i):
            l, c = i // NC, i % NC
            p = i % AHEAD
            for sem in (ag_r.at[0, i, 0], ag_s.at[0, p, 0]):
                wait(wgu_h.at[0, 0, 0, 0, pl.ds(0, S - 1)], sem)
            wait(wgu_h.at[0, 0, 0, 0, 0], ag_loc.at[p, 0])

            @pl.when(par == 0)
            def _():
                w = wgu_h.at[0, l, c, :, py]
                for r in range(1, S):
                    send(w, w, ag_s.at[1, p, 0], ag_r.at[1, i, 0], at(px, py + r))

            @pl.when(par == 1)
            def _():
                w = wgu_h.at[1, l, c, px]
                for r in range(1, S):
                    send(w, w, ag_s.at[1, p, 0], ag_r.at[1, i, 0], at(px + r, py))

            @with_down(i)
            def _():
                for sem in (ag_r.at[0, i, 1], ag_s.at[0, p, 1]):
                    wait(wd_h.at[0, pl.ds(0, (S - 1) * HW)], sem)
                wait(wd_h.at[0, pl.ds(0, HW)], ag_loc.at[p, 1])
                for k in range(S):
                    v = wd_h.at[l, rows((1 - par) * (S * k + py) + par * (S * px + k), c)]
                    for r in range(1, S):
                        send(v, v, ag_s.at[1, p, 1], ag_r.at[1, i, 1], at(px + r * par, py + r * (1 - par)))

        def ag3(i):
            l, c = i // NC, i % NC
            p = i % AHEAD
            for sem in (ag_r.at[1, i, 0], ag_s.at[1, p, 0]):
                wait(wgu_h.at[0, 0, 0, pl.ds(0, S - 1)], sem)
            w = wgu_h.at[par, l, c]
            send(w, w, ag_s.at[2, p, 0], ag_r.at[2, i, 0], partner)

            @with_down(i - 1)
            def _():
                for sem in (ag_r.at[1, i - 1, 1], ag_s.at[1, (i - 1) % AHEAD, 1]):
                    wait(wd_h.at[0, pl.ds(0, S * (S - 1) * HW)], sem)
                for d in range(n):
                    v = wd_h.at[l, rows(d, (i - 1) % NC)]
                    send(v, v, ag_s.at[2, (i - 1) % AHEAD, 1], ag_r.at[2, i - 1, 1], partner)

        def ag4(i):
            for sem in (ag_r.at[2, i, 0], ag_s.at[2, i % AHEAD, 0]):
                wait(one_chunk, sem)

            @with_down(i - 1)
            def _():
                for sem in (ag_r.at[2, i - 1, 1], ag_s.at[2, (i - 1) % AHEAD, 1]):
                    wait(wd_h.at[0, pl.ds(0, n * HW)], sem)

        pltpu.make_async_copy(wg, wl.at[0], sm.at[0]).start()
        pltpu.make_async_copy(wu, wl.at[1], sm.at[1]).start()
        for l in range(L):
            for q in range(RF // HW):
                pltpu.make_async_copy(wd.at[l, pl.ds(q * HW, HW)], wdl.at[l, q], sm.at[2]).start()
        barrier = pltpu.get_barrier_semaphore()
        for r in range(1, n):
            pl.semaphore_signal(barrier, inc=1, device_id={"dp": (me + r) % n}, device_id_type=MESH)
        pl.semaphore_signal(barrier, inc=1, device_id=partner, device_id_type=MESH)

        def fetch(b):
            return pltpu.make_async_copy(x.at[blocks(b, TD)], xs.at[b % SLOTS], sx.at[b % SLOTS])

        def turn(b, _):
            pl.when(b + 1 < NB)(lambda: fetch(b + 1).start())
            fetch(b).wait()
            aT[:, blocks(b, TD)] = xs[b % SLOTS].T
            before = blocks((b + NB - 1) % NB, TD)
            norm(aT.at[:, before], aT.at[:, before])
            return 0

        fetch(0).start()
        wait(wl.at[0], sm.at[0])
        wait(wl.at[1], sm.at[1])
        wait(wdl, sm.at[2])
        pl.semaphore_wait(barrier, n)
        for i in range(3):
            ag1(i)
        lax.fori_loop(0, 3, turn, 0)
        ag2(0)
        lax.fori_loop(3, 4, turn, 0)
        ag2(1)
        ag2(2)
        ag1(3)
        lax.fori_loop(4, NB, turn, 0)
        norm(aT.at[:, blocks(NB - 1, TD)], aT.at[:, blocks(NB - 1, TD)])
        acc[...] = jnp.zeros_like(acc)
        ag3(0)
        ag4(0)
        load_w(0, 0)
        pltpu.make_async_copy(aT, a0_h, sm.at[0]).start()
        ag3(1)

        def load_down(third):
            some = blocks(third, FF // NW)
            return pltpu.make_async_copy(wd_h.at[0, some], w_down.at[some], swd.at[0])

        def down():
            fetch(0).start()
            for third in range(NW):
                load_down(third).wait()
            wait(aT, sm.at[0])

            def save(b):
                return pltpu.make_async_copy(h1s.at[b % SLOTS], h1_h.at[:, blocks(b, TD)], sh.at[b % SLOTS])

            def normed(b):
                scl[:, blocks(b, TD)] = norm(h1s.at[b % SLOTS], aT.at[:, blocks(b, TD)])

            def block(b, _):
                @pl.when(b + 1 < NB)
                def _():
                    fetch(b + 1).start()

                fetch(b).wait()
                pl.when(b >= 2)(lambda: save(b - 2).wait())
                out = dot(w_down[...], hiddenT[:, blocks(b, TD)], TN).astype(bf16)
                normed((b + NB - 1) % NB)
                h1s[b % SLOTS] = xs[b % SLOTS].T + out
                save(b).start()
                return 0

            lax.fori_loop(0, NB, block, 0)
            normed(NB - 1)
            for b in range(NB - 2, NB):
                save(b).wait()

        def save_hidden(i):
            return pltpu.make_async_copy(hiddenT.at[cols(i % NC)], hid_h.at[i // NC, cols(i % NC)], shid.at[i % SLOTS])

        def part_of_dy(q):
            return q % (T // LANES)

        def fetch_dy(q):
            return pltpu.make_async_copy(dy.at[pl.ds(pl.multiple_of(part_of_dy(q) * LANES, LANES), LANES)], dys.at[q % SLOTS], sdy.at[q % SLOTS])

        fetch_dy(0).start()

        def chunk(i, _):
            l, c = i // NC, i % NC
            pl.when((c == 0) & (l > 0))(down)
            slot = i % SLOTS
            wait_w(slot)
            pl.when(i + 3 < NI)(lambda: ag2(i + 3))
            pl.when(i + 4 < NI)(lambda: ag1(i + 4))

            @pl.when(i == NC - 1)
            def _():
                for third in range(NW):
                    load_down(third).start()

            def block(j, _):
                @pl.when((j == NJ - 1) & (i + 1 < NI))
                def _():
                    ag4(i + 1)
                    load_w(i + 1, 1 - slot)

                pl.when((j == NJ - 1) & (i + 2 < NI))(lambda: ag3(i + 2))
                q = i * NJ + j
                pl.when(q + 1 < NI * NJ)(lambda: fetch_dy(q + 1).start())
                fetch_dy(q).wait()

                @pl.when(i > 0)
                def _():
                    wait(stage.at[j], s_stage.at[j])

                t = blocks(j, TB)
                r = dot(wcomb[slot].reshape(D, WIDE), aT[:, t], TN)
                gate, up = r[:CH], r[CH:]
                sig = 0.5 * jnp.tanh(0.5 * gate) + 0.5
                silu = gate * sig
                stage[j, :CH, :] = silu
                stage[j, CH:, :] = up * (sig + silu * (1.0 - sig))
                hiddenT[cols(c), t] = (silu * up).astype(bf16)
                dyT[:, pl.ds(pl.multiple_of(part_of_dy(q) * LANES, LANES), LANES)] = dys[q % SLOTS].T
                pltpu.make_async_copy(stage.at[j], st_h.at[l, c, :, t], s_stage.at[j]).start()
                return 0

            lax.fori_loop(0, NJ, block, 0)
            pl.when(i >= 2)(lambda: save_hidden(i - 2).wait())
            save_hidden(i).start()
            return 0

        lax.fori_loop(0, NI, chunk, 0)
        load_wd(*item(0), 0).start()
        for j in range(NJ):
            wait(stage.at[j], s_stage.at[j])
            load_stage(0, j).start()
        load_w(item(0)[0] * NC + item(0)[1], 0)
        for i in range(NI - SLOTS, NI):
            save_hidden(i).wait()

    dma = pltpu.SemaphoreType.DMA
    pl.run_scoped(
        forward,
        vmem((FF, T), bf16),
        vmem((FF, D), bf16),
        vmem((SLOTS, TD, D), bf16),
        vmem((SLOTS, LANES, D), bf16),
        vmem((SLOTS, D, TD), bf16),
        vmem((SLOTS, L, R, FF), bf16),
        vmem((L, RF // HW, HW, D), bf16),
        dma((SLOTS,)),
        dma((SLOTS,)),
    )

    def backward(daT, big, hid, Fg, Fd, s1, sb, s2, o1, o2, la, sh):
        pieces = [(pl.ds(0, R), pl.ds(0, CH))] + [(pl.ds(R + i * SUB, SUB), pl.ds(0, min(CH, D - i * CH))) for i in range(pl.cdiv(D, CH))]

        def down_piece(i):
            return pl.ds((i - 1) * CH, pieces[i][1].size)

        def places(h, a, b):
            return (a, b) if h == 0 else (b, a)

        def own_sums(p, d, h, i):
            return Fd[p, d, pl.ds(h * SUB, SUB), down_piece(i)] if i else Fg[p, d, :, pl.ds(h * CH, CH)]

        def near(u, a):
            return a + 1 - a % PAIR * PAIR if u == 0 else S - 1 - a

        def far(u, a):
            return near(1 - u, a)

        def rs_send(k):
            l, c = item(k)
            p = k % SLOTS
            for h in range(HALVES):
                a, b = places(h, px, py)
                for u in range(HALVES):
                    src = s1.at[p, h, pl.ds(1 + (a + u) % PAIR, PAIR), pl.ds(u * PAIR, PAIR)]
                    send(src, rA.at[l, c, h, u], rs_s.at[0, p], rs_r.at[k, 0], at(*places(h, near(u, a), b)))

        def rs_pass_b(k):
            p = k % SLOTS

            @pl.when((k >= 2) & (k < NI + 2))
            def _():
                for h in range(HALVES):
                    a, b = places(h, px, py)
                    for u in range(HALVES):
                        src = sb.at[p, h, pl.ds(u * PAIR, PAIR)]
                        send(src, lb.at[(k - 2) % NW, h, u], rs_s.at[1, p], rs_r.at[k - 2, 1], at(*places(h, far(u, a), b)))

        def rs_pass_2(k):
            p = k % SLOTS

            @pl.when((k >= 3) & (k < NI + 3))
            def _():
                for h in range(HALVES):
                    a, b = places(h, px, py)
                    for r in range(1, S):
                        to = at(*places(h, a, b + r))
                        send(s2.at[1 - p, h, (b + r) % S], l2.at[1 - p, h, S - 1 - r], rs_s.at[2, 1 - p], rs_r.at[k - 3, 2], to)

        def rs_early(k):
            @pl.when((k >= 2) & (k < NI + 2))
            def _():
                l, c = item(k - 2)
                wait(rA.at[l, c], rs_r.at[k - 2, 0])
                wait(rA.at[l, c], rs_s.at[0, k % SLOTS])
                pltpu.make_async_copy(rA.at[l, c], la, rs_l).start()

        def rs_arrived_a(k):
            pl.when((k >= 2) & (k < NI + 2))(lambda: wait(la, rs_l))

        def rs_arrived(k):
            for stage_of, here in ((1, lb), (2, l2)):
                q = k - 2 - stage_of

                @pl.when((q >= 0) & (q < NI))
                def _():
                    wait(here.at[0], rs_r.at[q, stage_of])
                    wait(here.at[0], rs_s.at[stage_of, q % SLOTS])

        def landed(k, lag, slots):
            any_yet = (k + NI + 4 - lag) // (NI + 4)
            return any_yet * ((k + NI - lag) % slots) + (1 - any_yet) * (slots - 1)

        def rs_sums(k):
            in_b, in_2 = landed(k, 3, NW), landed(k, 4, SLOTS)
            q = (k + NI - 4) % NI
            l, c = item(q)
            p = k % SLOTS
            squares = jnp.zeros(TILE, f32)
            for h in range(HALVES):
                for i, piece in enumerate(pieces):
                    total = o2[(h,) + piece]
                    for j in range(S - 1):
                        total += l2[(in_2, h, j) + piece].astype(f32)
                    g = total.astype(bf16)
                    if i:
                        gd[l, pl.ds(pl.multiple_of(c * RC + h * SUB, SUB), SUB), down_piece(i)] = g
                    else:
                        (gg, gu)[h][l, :, cols(c)] = g
                    g = g.astype(f32)
                    g = g * g
                    for a in range(g.shape[0] // SUB):
                        for b in range(g.shape[1] // LANES):
                            squares += g[a * SUB : (a + 1) * SUB, b * LANES : (b + 1) * LANES]
            acc[...] += jnp.where(k >= 4, squares, 0.0)
            for h in range(HALVES):
                a, b = places(h, px, py)
                for i, piece in enumerate(pieces):
                    for s in range(S):
                        total = o1[(1 - p, h, s) + piece] + lb[(in_b, h, s // PAIR, s % PAIR) + piece].astype(f32)
                        s2[(1 - p, h, s) + piece] = total.astype(bf16)
                        own = jnp.where(b == s, total, own) if s else total
                    o2[(h,) + piece] = own

        def rs_sums_a(k):
            p = k % SLOTS
            for h in range(HALVES):
                a, b = places(h, px, py)
                for i, piece in enumerate(pieces):
                    for s in range(S):
                        u = s // PAIR
                        ours = (a + 1 + u) % PAIR
                        for keep_it, first, index in ((True, a, ours), (False, far(u, a), 1 - ours)):
                            ix, iy = places(h, first, s)
                            total = own_sums(p, ix * S + iy, h, i) + la[(h, u, index, s % PAIR) + piece].astype(f32)
                            if keep_it:
                                o1[(p, h, s) + piece] = total
                            else:
                                sb[(p, h, s) + piece] = total.astype(bf16)

        def load_hidden(k):
            l, c = item(k)
            for d in range(n):
                rows = hid_h.at[l, pl.ds(pl.multiple_of(d * RF + c * RC, 8), RC)]
                pltpu.make_async_copy(rows, hid.at[pl.ds(d * RC, RC)], shid.at[0]).start()

        def at_rows(slot, row, size):
            return pl.ds(row % CH, size), pl.ds(pl.multiple_of(slot * (T // 2) + row // CH * TD, TD), TD)

        def each_h(b, do):
            size = LANES
            for row in range(0, D, size):
                do(pltpu.make_async_copy(h1_h.at[pl.ds(row, size), blocks(b, TD)], hid.at[at_rows(b % SLOTS, row, size)], sh.at[b % SLOTS]))

        def through_norm():
            def block(b, _):
                t = blocks(b, TD)
                pl.when((b > 0) & (b + 1 < NB))(lambda: each_h(b + 1, lambda copy: copy.start()))
                each_h(b, lambda copy: copy.wait())

                def both(g):
                    rows = pl.ds(g, PACK)
                    return daT[rows, t].astype(bf16).astype(f32), hid[at_rows(b % SLOTS, g, PACK)].astype(f32)

                along = jnp.zeros((SUB, TD), f32)
                for g in range(0, D, PACK):
                    da, wide = both(g)
                    wide = da * wide
                    along += wide[:SUB] + wide[SUB:]
                scale = scl[:, t]
                along = jnp.sum(along, axis=0, keepdims=True) * (scale * scale * scale) * (-1 / D)
                for g in range(0, D, PACK):
                    da, wide = both(g)
                    dyT[pl.ds(g, PACK), t] += (da * scale + wide * along).astype(bf16)
                return 0

            lax.fori_loop(0, NB, block, 0)
            load_hidden(NC)

        load_hidden(0)

        def one(k, _):
            l, c = item(k)
            slot = k % SLOTS

            @pl.when(k + 1 < NI)
            def _():
                load_wd(*item(k + 1), 1 - slot).start()

            @pl.when(k == NC)
            def _():
                through_norm()
                wait(aT, sm.at[0])

            @pl.when(k + 1 < NC)
            def _():
                load_w((L - 1) * NC + k + 1, 1 - slot)

            rs_early(k)
            load_wd(l, c, slot).wait()

            def block(j, _):
                load_stage(k, j).wait()
                t = blocks(j, TB)
                dh = dot(wdc[slot], dyT[:, t]).astype(bf16).astype(f32)
                big[:CH, t] = (dh * stage[j, CH:, :]).astype(bf16)
                big[CH:, t] = (dh * stage[j, :CH, :]).astype(bf16)
                pl.when(k + 1 < NI)(lambda: load_stage(k + 1, j).start())
                return 0

            lax.fori_loop(0, NJ, block, 0)
            rs_arrived_a(k)
            rs_arrived(k)
            rs_sums(k)
            rs_sums_a(k)

            def to_send(d, h):
                first, second = places(h, d // S, d % S)
                return slot, h, (first + S - (px, py)[h]) % S, second

            wide = dot(aT[...], big[...], NT)
            for d in range(n):
                block = wide[d * R : (d + 1) * R]
                Fg[slot, d] = block
                for h in range(HALVES):
                    s1[to_send(d, h) + pieces[0]] = block[:, h * CH : (h + 1) * CH].astype(bf16)
            rs_pass_b(k)
            rs_pass_2(k)
            pl.when(k == NC - 1)(lambda: pltpu.make_async_copy(a0_h, aT, sm.at[0]).start())
            wait(hid, shid.at[0])

            @pl.when(k < NI)
            def _():
                down = dot(dyT[...], hid[...], NT).T
                for d in range(n):
                    block = down[d * RC : (d + 1) * RC]
                    Fd[slot, d] = block
                    for h in range(HALVES):
                        for i in range(1, len(pieces)):
                            columns = down_piece(i)
                            some = block[h * SUB : (h + 1) * SUB, columns.start : columns.start + columns.size]
                            s1[to_send(d, h) + pieces[i]] = some.astype(bf16)

            rs_send(k)
            pl.when((k + 1 < NI) & (k + 1 != NC))(lambda: load_hidden(k + 1))

            @pl.when(k + 1 == NC)
            def _():
                for b in range(2):
                    each_h(b, lambda copy: copy.start())


            def into(first):
                wait_w(slot)
                da = dot(wcomb[slot].reshape(D, WIDE), big[...])
                daT[...] = da if first else daT[...] + da

            pl.when(k == 0)(lambda: into(True))
            pl.when((k > 0) & (k < NC))(lambda: into(False))
            return 0

        lax.fori_loop(0, NI, one, 0)

        def rest(k, _):
            rs_early(k)
            rs_arrived_a(k)
            rs_sums_a(k)
            rs_pass_b(k)
            rs_arrived(k)
            rs_sums(k)
            rs_pass_2(k)
            return 0

        lax.fori_loop(NI, NI + 4, rest, 0)

    pl.run_scoped(
        backward,
        vmem((D, T), f32),
        vmem((WIDE, T), bf16),
        vmem((n * RC, T), bf16),
        vmem((SLOTS, n, R, WIDE), f32),
        vmem((SLOTS, n, RC, D), f32),
        vmem((SLOTS, HALVES, S, S, RB, CH), bf16),
        vmem((SLOTS, HALVES, S, RB, CH), bf16),
        vmem((SLOTS, HALVES, S, RB, CH), bf16),
        vmem((SLOTS, HALVES, S, RB, CH), f32),
        vmem((HALVES, RB, CH), f32),
        vmem(rA.shape[2:], bf16),
        dma((SLOTS,)),
    )

    results = [pltpu.make_async_copy(here, to, sm.at[i]) for i, (here, to) in enumerate(((gg, gg_h), (gu, gu_h), (gd, gd_h)))]
    for copy in results:
        copy.start()
    sst[...] = acc[...]
    ssr[me] = acc[...]
    for r in range(1, n):
        send(sst, ssr.at[me], ss_s, ss_r, {"dp": (me + r) % n})
    wait(ssr.at[pl.ds(0, n - 1)], ss_r)
    wait(ssr.at[pl.ds(0, n - 1)], ss_s)
    total = ssr[0]
    for d in range(1, n):
        total += ssr[d]
    ss[...] = total
    for copy in results:
        copy.wait()


def solution(mesh):
    n = mesh.shape["dp"]
    S = math.isqrt(n)

    def step(x, dy, *arrays):
        weights, m, v = (arrays[i : i + 3] for i in (0, 3, 6))
        L, R, FF = weights[0].shape
        RF, D = weights[2].shape[1:]
        T = x.shape[1]
        NC = FF // CH
        RB = R + SUB * pl.cdiv(D, CH)
        NJ = T // TB
        sds = jax.ShapeDtypeStruct
        vmem, dma = pltpu.VMEM, pltpu.SemaphoreType.DMA
        outs = [
            (sds((L, R, FF), bf16), pl.ANY),
            (sds((L, R, FF), bf16), pl.ANY),
            (sds((L, RF, D), bf16), pl.ANY),
            (sds(TILE, f32), pltpu.VMEM),
            (sds((2, L, NC, S, S, R, CH), bf16), pl.ANY),
            (sds((L, FF, D), bf16), pl.ANY),
            (sds((L, NC, WIDE, T), f32), pl.ANY),
            (sds((L, FF, T), bf16), pl.ANY),
            (sds((D, T), bf16), pl.ANY),
            (sds((D, T), bf16), pl.ANY),
            (sds((L, NC, HALVES, HALVES, PAIR, PAIR, RB, CH), bf16), pl.ANY),
        ]
        scratch = [
            vmem((L, R, FF), bf16),
            vmem((L, R, FF), bf16),
            vmem((L, RF, D), bf16),
            vmem((SLOTS, D, T), bf16),
            vmem((NJ, WIDE, TB), f32),
            vmem((SLOTS, S, S, R, WIDE), bf16),
            vmem((SLOTS, CH, D), bf16),
            vmem((1, T), f32),
            vmem(TILE, f32),
            vmem(TILE, f32),
            vmem((n,) + TILE, f32),
            vmem((3, HALVES, HALVES, PAIR, RB, CH), bf16),
            vmem((SLOTS, HALVES, S - 1, RB, CH), bf16),
            dma((SLOTS,)),
            dma((2, 2)),
            dma((SLOTS,)),
            dma((NJ,)),
            dma((SLOTS,)),
            dma((3,)),
            dma((AHEAD, 2)),
            dma((3, AHEAD, 2)),
            dma((3, L * NC, 2)),
            dma((3, SLOTS)),
            dma((L * NC, 3)),
            dma(()),
            dma(()),
            dma(()),
        ]
        flops = 15 * 2 * T * D * FF
        done = pl.pallas_call(
            lambda *refs: step_kernel(n, *refs),
            in_specs=[pl.BlockSpec(memory_space=pl.ANY)] * 5,
            out_specs=[pl.BlockSpec(memory_space=space) for _, space in outs],
            out_shape=[shape for shape, _ in outs],
            scratch_shapes=scratch,
            compiler_params=pltpu.CompilerParams(collective_id=0, has_side_effects=True, vmem_limit_bytes=VMEM_BYTES),
            cost_estimate=pl.CostEstimate(flops=flops, bytes_accessed=400 << 20, transcendentals=0),
            name="train_step",
        )(x[0], dy[0], *weights)
        gradients = done[:3]
        count = n * sum(g.size for g in gradients)
        old = [array for g, w, m_, v_ in zip(gradients, weights, m, v, strict=True) for array in (g, w, m_, v_)]
        new = pl.pallas_call(
            lambda *refs: adamw_kernel(count, *refs),
            in_specs=[pl.BlockSpec(memory_space=pltpu.VMEM)] + [pl.BlockSpec(memory_space=pl.ANY)] * len(old),
            out_specs=[pl.BlockSpec(memory_space=pl.ANY)] * (len(weights) * 3),
            out_shape=[sds(a.shape, a.dtype) for w, m_, v_ in zip(weights, m, v, strict=True) for a in (w, m_, v_)],
            scratch_shapes=[vmem(a.shape, a.dtype) for a in old] + [dma((len(old),))],
            compiler_params=pltpu.CompilerParams(vmem_limit_bytes=VMEM_BYTES),
            name="adamw",
        )(done[3], *old)
        return tuple(new[i] for which in range(3) for i in range(which, len(new), 3))

    states, cut = P(("rep", "dp"), None, None), P(None, "dp", None)
    return jax.shard_map(
        step,
        mesh=mesh,
        in_specs=(states, states) + (cut,) * 9,
        out_specs=(P("rep", "dp", None),) * 9,
        check_vma=False,
    )
```

```python
import math

import jax
import jax.numpy as jnp
from jax import lax
from jax.experimental import pallas as pl
from jax.experimental.pallas import tpu as pltpu
from jax.sharding import PartitionSpec as P

bf16, f32 = jnp.bfloat16, jnp.float32
MESH = pl.DeviceIdType.MESH
CH = 256
TB = 2048
TD = 2 * CH
TILE = SUB, LANES = 8, 128
PACK = 2 * SUB
WIDE = 2 * CH
VMEM_BYTES = 67043328
AHEAD = 4
SLOTS = HALVES = KINDS = PAIR = 2
NN = (((1,), (0,)), ((), ()))
NT = (((1,), (1,)), ((), ()))
TN = (((0,), (0,)), ((), ()))


def dot(a, b, dims=NN):
    return lax.dot_general(a, b, dims, preferred_element_type=f32)


def adamw_kernel(count, squares, *refs):
    groups = len(refs) // 11
    arrays, out, held, sems = refs[: groups * 4], refs[groups * 4 : groups * 7], refs[groups * 7 : -1], refs[-1]
    for i, (array, here) in enumerate(zip(arrays, held, strict=True)):
        pltpu.make_async_copy(array, here, sems.at[i]).start()
    total = jnp.sum(squares[...], keepdims=True)
    factor = jnp.minimum(1.0, 0.5 * lax.rsqrt(total / count + 1e-30))
    stores = []
    for group in range(groups):
        g_ref, w_ref, m_ref, v_ref = held[group * 4 : group * 4 + 4]
        for i in range(group * 4, group * 4 + 4):
            pltpu.make_async_copy(arrays[i], held[i], sems.at[i]).wait()
        def one_layer(at, _):
            g = g_ref[at].astype(f32) * factor
            w = w_ref[at].astype(f32)
            m = 0.9 * m_ref[at] + 0.1 * g
            v = 0.95 * v_ref[at] + 0.05 * g * g
            step = m * lax.rsqrt(v + 1e-8) + 0.1 * w
            w_ref[at] = (w - 0.02 * step).astype(bf16)
            m_ref[at] = m
            v_ref[at] = v
            return 0

        lax.fori_loop(0, g_ref.shape[0], one_layer, 0)
        for i, here in enumerate((w_ref, m_ref, v_ref)):
            stores.append(pltpu.make_async_copy(here, out[group * 3 + i], sems.at[group * 4 + i]))
            stores[-1].start()
    for copy in stores:
        copy.wait()


def step_kernel(n, x, dy, wg, wu, wd, *refs):
    (gg_h, gu_h, gd_h, ss, wgu_h, wd_h, st_h, hid_h, a0_h, h1_h, rA) = refs[:11]
    (gg, gu, gd, act, stage, wcomb, wdc, scl, acc, sst, ssr, lb, l2) = refs[11:24]
    (sx, sw, swd, s_stage, shid, sm, ag_loc, ag_s, ag_r, rs_s, rs_r, rs_l, ss_s, ss_r) = refs[24:]
    L, R, FF = wg.shape
    RF, D = wd.shape[1:]
    T = x.shape[0]
    S = math.isqrt(n)
    NC = FF // CH
    NI = L * NC
    NJ = T // TB
    NB = T // TD
    NW = 3
    HW = RF // 2 // NW
    RC = RF // NC
    RB = R + SUB * pl.cdiv(D, CH)
    me, rep = lax.axis_index("dp"), lax.axis_index("rep")
    px, py = me // S, me % S
    par = rep % SLOTS
    one_chunk = wgu_h.at[0, 0, 0]
    partner = {"rep": rep + 1 - 2 * par, "dp": me}
    aT, dyT = act.at[0], act.at[1]
    vmem = pltpu.VMEM

    def at(ix, iy):
        return {"dp": (ix % S) * S + iy % S}

    def send(src, dst, s, r, to):
        pltpu.make_async_remote_copy(src_ref=src, dst_ref=dst, send_sem=s, recv_sem=r, device_id=to, device_id_type=MESH).start()

    def wait(ref, sem):
        pltpu.make_async_copy(ref, ref, sem).wait()

    def cols(c):
        return pl.ds(pl.multiple_of(c * CH, CH), CH)

    def blocks(b, size):
        return pl.ds(pl.multiple_of(b * size, size), size)

    def load_w(i, slot):
        for h in range(HALVES):
            pltpu.make_async_copy(wgu_h.at[h, i // NC, i % NC], wcomb.at[slot, :, :, :, pl.ds(h * CH, CH)], sw.at[slot, h]).start()

    def wait_w(slot):
        for h in range(HALVES):
            wait(one_chunk, sw.at[slot, h])

    def load_wd(l, c, slot):
        return pltpu.make_async_copy(wd_h.at[l, cols(c)], wdc.at[slot], swd.at[slot])

    def item(k):
        return L - 1 - k // NC, k % NC

    def load_stage(k, j):
        l, c = item(k)
        return pltpu.make_async_copy(st_h.at[l, c, :, blocks(j, TB)], stage.at[j], s_stage.at[j])

    def norm(src, dst):
        def rows(g):
            return pl.ds(g * PACK, PACK)

        total = jnp.zeros((SUB, src.shape[1]), f32)
        for g in range(D // (PACK)):
            wide = src[rows(g), :].astype(f32)
            wide = wide * wide
            total += wide[:SUB] + wide[SUB:]
        scale = lax.rsqrt(jnp.sum(total, axis=0, keepdims=True) / D + 1e-6)
        for g in range(D // (PACK)):
            dst[rows(g), :] = (src[rows(g), :].astype(f32) * scale).astype(bf16)
        return scale

    def forward(hiddenT, w_down, xs, dys, h1s, wl, wdl, sh, sdy):
        def with_down(i):
            return pl.when((i % NC >= NW) & (i % NC % PAIR == 1))

        def rows(d, c):
            return pl.ds(pl.multiple_of(d * RF + par * (RF // 2) + (c - NW) // PAIR * HW, 8), HW)

        def ag1(i):
            l, c = i // NC, i % NC
            p = i % AHEAD
            src, own = wl.at[par, l, :, cols(c)], wgu_h.at[par, l, c, px, py]
            for r in range(1, S):
                send(src, own, ag_s.at[0, p, 0], ag_r.at[0, i, 0], at(px + r * (1 - par), py + r * par))
            pltpu.make_async_copy(src, own, ag_loc.at[p, 0]).start()

            @with_down(i)
            def _():
                src, own = wdl.at[l, par * NW + (c - NW) // PAIR], wd_h.at[l, rows(me, c)]
                for r in range(1, S):
                    send(src, own, ag_s.at[0, p, 1], ag_r.at[0, i, 1], at(px + r * (1 - par), py + r * par))
                pltpu.make_async_copy(src, own, ag_loc.at[p, 1]).start()

        def ag2(i):
            l, c = i // NC, i % NC
            p = i % AHEAD
            for sem in (ag_r.at[0, i, 0], ag_s.at[0, p, 0]):
                wait(wgu_h.at[0, 0, 0, 0, pl.ds(0, S - 1)], sem)
            wait(wgu_h.at[0, 0, 0, 0, 0], ag_loc.at[p, 0])

            @pl.when(par == 0)
            def _():
                w = wgu_h.at[0, l, c, :, py]
                for r in range(1, S):
                    send(w, w, ag_s.at[1, p, 0], ag_r.at[1, i, 0], at(px, py + r))

            @pl.when(par == 1)
            def _():
                w = wgu_h.at[1, l, c, px]
                for r in range(1, S):
                    send(w, w, ag_s.at[1, p, 0], ag_r.at[1, i, 0], at(px + r, py))

            @with_down(i)
            def _():
                for sem in (ag_r.at[0, i, 1], ag_s.at[0, p, 1]):
                    wait(wd_h.at[0, pl.ds(0, (S - 1) * HW)], sem)
                wait(wd_h.at[0, pl.ds(0, HW)], ag_loc.at[p, 1])
                for k in range(S):
                    v = wd_h.at[l, rows((1 - par) * (S * k + py) + par * (S * px + k), c)]
                    for r in range(1, S):
                        send(v, v, ag_s.at[1, p, 1], ag_r.at[1, i, 1], at(px + r * par, py + r * (1 - par)))

        def ag3(i):
            l, c = i // NC, i % NC
            p = i % AHEAD
            for sem in (ag_r.at[1, i, 0], ag_s.at[1, p, 0]):
                wait(wgu_h.at[0, 0, 0, pl.ds(0, S - 1)], sem)
            w = wgu_h.at[par, l, c]
            send(w, w, ag_s.at[2, p, 0], ag_r.at[2, i, 0], partner)

            @with_down(i - 1)
            def _():
                for sem in (ag_r.at[1, i - 1, 1], ag_s.at[1, (i - 1) % AHEAD, 1]):
                    wait(wd_h.at[0, pl.ds(0, S * (S - 1) * HW)], sem)
                for d in range(n):
                    v = wd_h.at[l, rows(d, (i - 1) % NC)]
                    send(v, v, ag_s.at[2, (i - 1) % AHEAD, 1], ag_r.at[2, i - 1, 1], partner)

        def ag4(i):
            for sem in (ag_r.at[2, i, 0], ag_s.at[2, i % AHEAD, 0]):
                wait(one_chunk, sem)

            @with_down(i - 1)
            def _():
                for sem in (ag_r.at[2, i - 1, 1], ag_s.at[2, (i - 1) % AHEAD, 1]):
                    wait(wd_h.at[0, pl.ds(0, n * HW)], sem)

        pltpu.make_async_copy(wg, wl.at[0], sm.at[0]).start()
        pltpu.make_async_copy(wu, wl.at[1], sm.at[1]).start()
        for l in range(L):
            for q in range(RF // HW):
                pltpu.make_async_copy(wd.at[l, pl.ds(q * HW, HW)], wdl.at[l, q], sm.at[2]).start()
        barrier = pltpu.get_barrier_semaphore()
        for r in range(1, n):
            pl.semaphore_signal(barrier, inc=1, device_id={"dp": (me + r) % n}, device_id_type=MESH)
        pl.semaphore_signal(barrier, inc=1, device_id=partner, device_id_type=MESH)

        def fetch(b):
            return pltpu.make_async_copy(x.at[blocks(b, TD)], xs.at[b % SLOTS], sx.at[b % SLOTS])

        def turn(b, _):
            pl.when(b + 1 < NB)(lambda: fetch(b + 1).start())
            fetch(b).wait()
            aT[:, blocks(b, TD)] = xs[b % SLOTS].T
            before = blocks((b + NB - 1) % NB, TD)
            norm(aT.at[:, before], aT.at[:, before])
            return 0

        fetch(0).start()
        wait(wl.at[0], sm.at[0])
        wait(wl.at[1], sm.at[1])
        wait(wdl, sm.at[2])
        pl.semaphore_wait(barrier, n)
        for i in range(3):
            ag1(i)
        lax.fori_loop(0, 3, turn, 0)
        ag2(0)
        ag1(3)
        lax.fori_loop(3, NB - 2, turn, 0)
        ag2(1)
        lax.fori_loop(NB - 2, NB, turn, 0)
        norm(aT.at[:, blocks(NB - 1, TD)], aT.at[:, blocks(NB - 1, TD)])
        acc[...] = jnp.zeros_like(acc)
        ag3(0)
        ag4(0)
        load_w(0, 0)
        ag2(2)
        pltpu.make_async_copy(aT, a0_h, sm.at[0]).start()
        ag3(1)

        def load_down(third):
            some = [cols(third * (NC // NW) + i) for i in range(NC // NW)]
            return [pltpu.make_async_copy(wd_h.at[0, rows_], w_down.at[rows_], swd.at[0]) for rows_ in some]

        def start_down(third):
            for copy in load_down(third):
                copy.start()

        def down():
            fetch(0).start()
            wait(w_down, swd.at[0])
            wait(aT, sm.at[0])

            def save(b):
                return pltpu.make_async_copy(h1s.at[b % SLOTS], h1_h.at[:, blocks(b, TD)], sh.at[b % SLOTS])

            def normed(b):
                scl[:, blocks(b, TD)] = norm(h1s.at[b % SLOTS], aT.at[:, blocks(b, TD)])

            def block(b, _):
                @pl.when(b + 1 < NB)
                def _():
                    fetch(b + 1).start()

                fetch(b).wait()
                pl.when(b >= 2)(lambda: save(b - 2).wait())
                out = dot(w_down[...], hiddenT[:, blocks(b, TD)], TN).astype(bf16)
                normed((b + NB - 1) % NB)
                h1s[b % SLOTS] = xs[b % SLOTS].T + out
                save(b).start()
                return 0

            lax.fori_loop(0, NB, block, 0)
            normed(NB - 1)
            for b in range(NB - 2, NB):
                save(b).wait()

        def save_hidden(i):
            return pltpu.make_async_copy(hiddenT.at[cols(i % NC)], hid_h.at[i // NC, cols(i % NC)], shid.at[i % SLOTS])

        def part_of_dy(q):
            return q % (T // LANES)

        def fetch_dy(q):
            return pltpu.make_async_copy(dy.at[pl.ds(pl.multiple_of(part_of_dy(q) * LANES, LANES), LANES)], dys.at[q % SLOTS], sdy.at[q % SLOTS])

        fetch_dy(0).start()

        def chunk(i, _):
            l, c = i // NC, i % NC
            pl.when((c == 0) & (l > 0))(down)
            slot = i % SLOTS
            wait_w(slot)
            pl.when(i + 3 < NI)(lambda: ag2(i + 3))
            pl.when(i + 4 < NI)(lambda: ag1(i + 4))

            def block(j, _):
                @pl.when((j == NJ - 1) & (i + 1 < NI))
                def _():
                    ag4(i + 1)
                    load_w(i + 1, 1 - slot)

                pl.when((j == NJ - 1) & (i + 2 < NI))(lambda: ag3(i + 2))
                q = i * NJ + j
                pl.when(q + 1 < NI * NJ)(lambda: fetch_dy(q + 1).start())
                fetch_dy(q).wait()
                for third in range(NW):
                    pl.when((i == NC - 1) & (j == (third + 1) // PAIR))(lambda: start_down(third))

                @pl.when(i > 0)
                def _():
                    wait(stage.at[j], s_stage.at[j])

                t = blocks(j, TB)
                r = dot(wcomb[slot].reshape(D, WIDE), aT[:, t], TN)
                gate, up = r[:CH], r[CH:]
                sig = 0.5 * jnp.tanh(0.5 * gate) + 0.5
                silu = gate * sig
                stage[j, :CH, :] = silu
                stage[j, CH:, :] = up * (sig + silu * (1.0 - sig))
                hiddenT[cols(c), t] = (silu * up).astype(bf16)
                dyT[:, pl.ds(pl.multiple_of(part_of_dy(q) * LANES, LANES), LANES)] = dys[q % SLOTS].T
                pltpu.make_async_copy(stage.at[j], st_h.at[l, c, :, t], s_stage.at[j]).start()
                return 0

            lax.fori_loop(0, NJ, block, 0)
            pl.when(i >= 2)(lambda: save_hidden(i - 2).wait())
            save_hidden(i).start()
            return 0

        lax.fori_loop(0, NI, chunk, 0)
        load_wd(*item(0), 0).start()
        for j in range(NJ):
            wait(stage.at[j], s_stage.at[j])
            load_stage(0, j).start()
        load_w(item(0)[0] * NC + item(0)[1], 0)
        for i in range(NI - SLOTS, NI):
            save_hidden(i).wait()

    dma = pltpu.SemaphoreType.DMA
    pl.run_scoped(
        forward,
        vmem((FF, T), bf16),
        vmem((FF, D), bf16),
        vmem((SLOTS, TD, D), bf16),
        vmem((SLOTS, LANES, D), bf16),
        vmem((SLOTS, D, TD), bf16),
        vmem((SLOTS, L, R, FF), bf16),
        vmem((L, RF // HW, HW, D), bf16),
        dma((SLOTS,)),
        dma((SLOTS,)),
    )

    def backward(daT, big, hid, Fg, Fd, s1, sb, s2, o1, o2, la, sh):
        pieces = [(pl.ds(0, R), pl.ds(0, CH))] + [(pl.ds(R + i * SUB, SUB), pl.ds(0, min(CH, D - i * CH))) for i in range(pl.cdiv(D, CH))]

        def down_piece(i):
            return pl.ds((i - 1) * CH, pieces[i][1].size)

        def places(h, a, b):
            return (a, b) if h == 0 else (b, a)

        def own_sums(p, d, h, i):
            return Fd[p, d, pl.ds(h * SUB, SUB), down_piece(i)] if i else Fg[p, d, :, pl.ds(h * CH, CH)]

        def near(u, a):
            return a + 1 - a % PAIR * PAIR if u == 0 else S - 1 - a

        def far(u, a):
            return near(1 - u, a)

        def rs_send(k):
            l, c = item(k)
            p = k % SLOTS
            for h in range(HALVES):
                a, b = places(h, px, py)
                for u in range(HALVES):
                    src = s1.at[p, h, pl.ds(1 + (a + u) % PAIR, PAIR), pl.ds(u * PAIR, PAIR)]
                    send(src, rA.at[l, c, h, u], rs_s.at[0, p], rs_r.at[k, 0], at(*places(h, near(u, a), b)))

        def rs_pass_b(k):
            p = k % SLOTS

            @pl.when((k >= 2) & (k < NI + 2))
            def _():
                for h in range(HALVES):
                    a, b = places(h, px, py)
                    for u in range(HALVES):
                        src = sb.at[p, h, pl.ds(u * PAIR, PAIR)]
                        send(src, lb.at[(k - 2) % NW, h, u], rs_s.at[1, p], rs_r.at[k - 2, 1], at(*places(h, far(u, a), b)))

        def rs_pass_2(k):
            p = k % SLOTS

            @pl.when((k >= 3) & (k < NI + 3))
            def _():
                for h in range(HALVES):
                    a, b = places(h, px, py)
                    for r in range(1, S):
                        to = at(*places(h, a, b + r))
                        send(s2.at[1 - p, h, (b + r) % S], l2.at[(k - 3) % AHEAD, h, S - 1 - r], rs_s.at[2, 1 - p], rs_r.at[k - 3, 2], to)

        def rs_early(k):
            @pl.when((k >= 2) & (k < NI + 2))
            def _():
                l, c = item(k - 2)
                wait(rA.at[l, c], rs_r.at[k - 2, 0])
                wait(rA.at[l, c], rs_s.at[0, k % SLOTS])
                pltpu.make_async_copy(rA.at[l, c], la, rs_l).start()

        def rs_arrived_a(k):
            pl.when((k >= 2) & (k < NI + 2))(lambda: wait(la, rs_l))

        def rs_arrived(k, stage_of, here):
            q = k - 2 - stage_of

            @pl.when((q >= 0) & (q < NI))
            def _():
                wait(here.at[0], rs_r.at[q, stage_of])
                wait(here.at[0], rs_s.at[stage_of, q % SLOTS])

        def landed(k, lag, slots):
            any_yet = (k + NI + 4 - lag) // (NI + 4)
            return any_yet * ((k + (slots - 1) * lag) % slots) + (1 - any_yet) * (slots - 1)

        def rs_last(k):
            q = (k + NI - 4) % NI
            l, c = item(q)
            landing = landed(k, 4, AHEAD)
            squares = jnp.zeros(TILE, f32)
            for h in range(HALVES):
                for i, piece in enumerate(pieces):
                    total = o2[(q % SLOTS, h) + piece]
                    for j in range(S - 1):
                        total += l2[(landing, h, j) + piece].astype(f32)
                    g = total.astype(bf16)
                    if i:
                        gd[l, pl.ds(pl.multiple_of(c * RC + h * SUB, SUB), SUB), down_piece(i)] = g
                    else:
                        (gg, gu)[h][l, :, cols(c)] = g
                    g = g.astype(f32)
                    g = g * g
                    for a in range(g.shape[0] // SUB):
                        for b in range(g.shape[1] // LANES):
                            squares += g[a * SUB : (a + 1) * SUB, b * LANES : (b + 1) * LANES]
            acc[...] += jnp.where(k >= 4, squares, 0.0)

        def rs_sums_b(k):
            p = (k + 1) % SLOTS
            landing = landed(k, 3, NW)
            for h in range(HALVES):
                a, b = places(h, px, py)
                for i, piece in enumerate(pieces):
                    for s in range(S):
                        total = o1[(p, h, s) + piece] + lb[(landing, h, s // PAIR, s % PAIR) + piece].astype(f32)
                        s2[(p, h, s) + piece] = total.astype(bf16)
                        own = jnp.where(b == s, total, own) if s else total
                    o2[(p, h) + piece] = own

        def rs_sums_a(k):
            p = k % SLOTS
            for h in range(HALVES):
                a, b = places(h, px, py)
                for i, piece in enumerate(pieces):
                    for s in range(S):
                        u = s // PAIR
                        ours = (a + 1 + u) % PAIR
                        for keep_it, first, index in ((True, a, ours), (False, far(u, a), 1 - ours)):
                            ix, iy = places(h, first, s)
                            total = own_sums(p, ix * S + iy, h, i) + la[(h, u, index, s % PAIR) + piece].astype(f32)
                            if keep_it:
                                o1[(p, h, s) + piece] = total
                            else:
                                sb[(p, h, s) + piece] = total.astype(bf16)

        def load_hidden(k):
            l, c = item(k)
            for d in range(n):
                rows = hid_h.at[l, pl.ds(pl.multiple_of(d * RF + c * RC, 8), RC)]
                pltpu.make_async_copy(rows, hid.at[pl.ds(d * RC, RC)], shid.at[0]).start()

        def at_rows(slot, row, size):
            return pl.ds(row % CH, size), pl.ds(pl.multiple_of(slot * (T // 2) + row // CH * TD, TD), TD)

        def each_h(b, do):
            size = LANES
            for row in range(0, D, size):
                do(pltpu.make_async_copy(h1_h.at[pl.ds(row, size), blocks(b, TD)], hid.at[at_rows(b % SLOTS, row, size)], sh.at[b % SLOTS]))

        def through_norm():
            def block(b, _):
                t = blocks(b, TD)
                pl.when((b > 0) & (b + 1 < NB))(lambda: each_h(b + 1, lambda copy: copy.start()))
                each_h(b, lambda copy: copy.wait())

                def both(g):
                    rows = pl.ds(g, PACK)
                    return daT[rows, t].astype(bf16).astype(f32), hid[at_rows(b % SLOTS, g, PACK)].astype(f32)

                along = jnp.zeros((SUB, TD), f32)
                for g in range(0, D, PACK):
                    da, wide = both(g)
                    wide = da * wide
                    along += wide[:SUB] + wide[SUB:]
                scale = scl[:, t]
                along = jnp.sum(along, axis=0, keepdims=True) * (scale * scale * scale) * (-1 / D)
                for g in range(0, D, PACK):
                    da, wide = both(g)
                    dyT[pl.ds(g, PACK), t] += (da * scale + wide * along).astype(bf16)
                return 0

            lax.fori_loop(0, NB, block, 0)
            load_hidden(NC)

        load_hidden(0)

        def one(k, _):
            l, c = item(k)
            slot = k % SLOTS

            @pl.when(k + 1 < NI)
            def _():
                load_wd(*item(k + 1), 1 - slot).start()

            @pl.when(k == NC)
            def _():
                through_norm()
                wait(aT, sm.at[0])

            @pl.when(k + 1 < NC)
            def _():
                load_w((L - 1) * NC + k + 1, 1 - slot)

            rs_early(k)
            load_wd(l, c, slot).wait()

            for j in range(NJ):
                load_stage(k, j).wait()
            dh = dot(wdc[slot], dyT[...])
            for j in range(NJ):
                t = slice(j * TB, (j + 1) * TB)
                part = dh[:, t].astype(bf16).astype(f32)
                big[:CH, t] = (part * stage[j, CH:, :]).astype(bf16)
                big[CH:, t] = (part * stage[j, :CH, :]).astype(bf16)

            @pl.when(k + 1 < NI)
            def _():
                for j in range(NJ):
                    load_stage(k + 1, j).start()

            rs_arrived_a(k)
            rs_arrived(k, 1, lb)
            rs_sums_b(k)
            rs_sums_a(k)

            def to_send(d, h):
                first, second = places(h, d // S, d % S)
                return slot, h, (first + S - (px, py)[h]) % S, second

            wide = dot(aT[...], big[...], NT)
            for d in range(n):
                block = wide[d * R : (d + 1) * R]
                Fg[slot, d] = block
                for h in range(HALVES):
                    s1[to_send(d, h) + pieces[0]] = block[:, h * CH : (h + 1) * CH].astype(bf16)
            rs_pass_b(k)
            pl.when(k == NC - 1)(lambda: pltpu.make_async_copy(a0_h, aT, sm.at[0]).start())
            wait(hid, shid.at[0])
            rs_arrived(k, 2, l2)

            @pl.when(k < NI)
            def _():
                rs_last(k)
                down = dot(dyT[...], hid[...], NT).T
                for d in range(n):
                    block = down[d * RC : (d + 1) * RC]
                    Fd[slot, d] = block
                    for h in range(HALVES):
                        for i in range(1, len(pieces)):
                            columns = down_piece(i)
                            some = block[h * SUB : (h + 1) * SUB, columns.start : columns.start + columns.size]
                            s1[to_send(d, h) + pieces[i]] = some.astype(bf16)

            rs_pass_2(k)
            rs_send(k)
            pl.when((k + 1 < NI) & (k + 1 != NC))(lambda: load_hidden(k + 1))

            @pl.when(k + 1 == NC)
            def _():
                for b in range(2):
                    each_h(b, lambda copy: copy.start())


            def into(first):
                wait_w(slot)
                da = dot(wcomb[slot].reshape(D, WIDE), big[...])
                daT[...] = da if first else daT[...] + da

            pl.when(k == 0)(lambda: into(True))
            pl.when((k > 0) & (k < NC))(lambda: into(False))
            return 0

        lax.fori_loop(0, NI, one, 0)

        def rest(k, _):
            rs_early(k)
            rs_arrived_a(k)
            rs_sums_a(k)
            rs_pass_b(k)
            rs_arrived(k, 1, lb)
            rs_sums_b(k)
            rs_pass_2(k)
            rs_arrived(k, 2, l2)
            rs_last(k)
            return 0

        lax.fori_loop(NI, NI + 4, rest, 0)

    pl.run_scoped(
        backward,
        vmem((D, T), f32),
        vmem((WIDE, T), bf16),
        vmem((n * RC, T), bf16),
        vmem((SLOTS, n, R, WIDE), f32),
        vmem((SLOTS, n, RC, D), f32),
        vmem((SLOTS, HALVES, S, S, RB, CH), bf16),
        vmem((SLOTS, HALVES, S, RB, CH), bf16),
        vmem((SLOTS, HALVES, S, RB, CH), bf16),
        vmem((SLOTS, HALVES, S, RB, CH), f32),
        vmem((SLOTS, HALVES, RB, CH), f32),
        vmem(rA.shape[2:], bf16),
        dma((SLOTS,)),
    )

    results = [pltpu.make_async_copy(here, to, sm.at[i]) for i, (here, to) in enumerate(((gg, gg_h), (gu, gu_h), (gd, gd_h)))]
    for copy in results:
        copy.start()
    sst[...] = acc[...]
    ssr[me] = acc[...]
    for r in range(1, n):
        send(sst, ssr.at[me], ss_s, ss_r, {"dp": (me + r) % n})
    wait(ssr.at[pl.ds(0, n - 1)], ss_r)
    wait(ssr.at[pl.ds(0, n - 1)], ss_s)
    total = ssr[0]
    for d in range(1, n):
        total += ssr[d]
    ss[...] = total
    for copy in results:
        copy.wait()


def solution(mesh):
    n = mesh.shape["dp"]
    S = math.isqrt(n)

    def step(x, dy, *arrays):
        weights, m, v = (arrays[i : i + 3] for i in (0, 3, 6))
        L, R, FF = weights[0].shape
        RF, D = weights[2].shape[1:]
        T = x.shape[1]
        NC = FF // CH
        RB = R + SUB * pl.cdiv(D, CH)
        NJ = T // TB
        sds = jax.ShapeDtypeStruct
        vmem, dma = pltpu.VMEM, pltpu.SemaphoreType.DMA
        outs = [
            (sds((L, R, FF), bf16), pl.ANY),
            (sds((L, R, FF), bf16), pl.ANY),
            (sds((L, RF, D), bf16), pl.ANY),
            (sds(TILE, f32), pltpu.VMEM),
            (sds((2, L, NC, S, S, R, CH), bf16), pl.ANY),
            (sds((L, FF, D), bf16), pl.ANY),
            (sds((L, NC, WIDE, T), f32), pl.ANY),
            (sds((L, FF, T), bf16), pl.ANY),
            (sds((D, T), bf16), pl.ANY),
            (sds((D, T), bf16), pl.ANY),
            (sds((L, NC, HALVES, HALVES, PAIR, PAIR, RB, CH), bf16), pl.ANY),
        ]
        scratch = [
            vmem((L, R, FF), bf16),
            vmem((L, R, FF), bf16),
            vmem((L, RF, D), bf16),
            vmem((SLOTS, D, T), bf16),
            vmem((NJ, WIDE, TB), f32),
            vmem((SLOTS, S, S, R, WIDE), bf16),
            vmem((SLOTS, CH, D), bf16),
            vmem((1, T), f32),
            vmem(TILE, f32),
            vmem(TILE, f32),
            vmem((n,) + TILE, f32),
            vmem((3, HALVES, HALVES, PAIR, RB, CH), bf16),
            vmem((AHEAD, HALVES, S - 1, RB, CH), bf16),
            dma((SLOTS,)),
            dma((2, 2)),
            dma((SLOTS,)),
            dma((NJ,)),
            dma((SLOTS,)),
            dma((3,)),
            dma((AHEAD, 2)),
            dma((3, AHEAD, 2)),
            dma((3, L * NC, 2)),
            dma((3, SLOTS)),
            dma((L * NC, 3)),
            dma(()),
            dma(()),
            dma(()),
        ]
        flops = 15 * 2 * T * D * FF
        done = pl.pallas_call(
            lambda *refs: step_kernel(n, *refs),
            in_specs=[pl.BlockSpec(memory_space=pl.ANY)] * 5,
            out_specs=[pl.BlockSpec(memory_space=space) for _, space in outs],
            out_shape=[shape for shape, _ in outs],
            scratch_shapes=scratch,
            compiler_params=pltpu.CompilerParams(
                collective_id=0,
                has_side_effects=True,
                vmem_limit_bytes=VMEM_BYTES,
            ),
            cost_estimate=pl.CostEstimate(flops=flops, bytes_accessed=400 << 20, transcendentals=0),
            name="train_step",
        )(x[0], dy[0], *weights)
        gradients = done[:3]
        count = n * sum(g.size for g in gradients)
        old = [array for g, w, m_, v_ in zip(gradients, weights, m, v, strict=True) for array in (g, w, m_, v_)]
        new = pl.pallas_call(
            lambda *refs: adamw_kernel(count, *refs),
            in_specs=[pl.BlockSpec(memory_space=pltpu.VMEM)] + [pl.BlockSpec(memory_space=pl.ANY)] * len(old),
            out_specs=[pl.BlockSpec(memory_space=pl.ANY)] * (len(weights) * 3),
            out_shape=[sds(a.shape, a.dtype) for w, m_, v_ in zip(weights, m, v, strict=True) for a in (w, m_, v_)],
            scratch_shapes=[vmem(a.shape, a.dtype) for a in old] + [dma((len(old),))],
            compiler_params=pltpu.CompilerParams(vmem_limit_bytes=VMEM_BYTES),
            name="adamw",
        )(done[3], *old)
        return tuple(new[i] for which in range(3) for i in range(which, len(new), 3))

    states, cut = P(("rep", "dp"), None, None), P(None, "dp", None)
    return jax.shard_map(
        step,
        mesh=mesh,
        in_specs=(states, states) + (cut,) * 9,
        out_specs=(P("rep", "dp", None),) * 9,
        check_vma=False,
    )
```

```python
import math

import jax
import jax.numpy as jnp
from jax import lax
from jax.experimental import pallas as pl
from jax.experimental.pallas import tpu as pltpu
from jax.sharding import PartitionSpec as P

bf16, f32 = jnp.bfloat16, jnp.float32
MESH = pl.DeviceIdType.MESH
CH = 256
TB = 2048
TD = 2 * CH
TILE = SUB, LANES = 8, 128
PACK = 2 * SUB
WIDE = 2 * CH
VMEM_BYTES = 67043328
AHEAD = 4
SLOTS = HALVES = KINDS = PAIR = 2
NN = (((1,), (0,)), ((), ()))
NT = (((1,), (1,)), ((), ()))
TN = (((0,), (0,)), ((), ()))


def dot(a, b, dims=NN):
    return lax.dot_general(a, b, dims, preferred_element_type=f32)


def adamw_kernel(count, squares, *refs):
    groups = len(refs) // 11
    arrays, out, held, sems = refs[: groups * 4], refs[groups * 4 : groups * 7], refs[groups * 7 : -1], refs[-1]
    for i, (array, here) in enumerate(zip(arrays, held, strict=True)):
        pltpu.make_async_copy(array, here, sems.at[i]).start()
    total = jnp.sum(squares[...], keepdims=True)
    factor = jnp.minimum(1.0, 0.5 * lax.rsqrt(total / count + 1e-30))
    stores = []
    for group in range(groups):
        g_ref, w_ref, m_ref, v_ref = held[group * 4 : group * 4 + 4]
        for i in range(group * 4, group * 4 + 4):
            pltpu.make_async_copy(arrays[i], held[i], sems.at[i]).wait()
        def one_layer(at, _):
            g = g_ref[at].astype(f32) * factor
            w = w_ref[at].astype(f32)
            m = 0.9 * m_ref[at] + 0.1 * g
            v = 0.95 * v_ref[at] + 0.05 * g * g
            step = m * lax.rsqrt(v + 1e-8) + 0.1 * w
            w_ref[at] = (w - 0.02 * step).astype(bf16)
            m_ref[at] = m
            v_ref[at] = v
            return 0

        lax.fori_loop(0, g_ref.shape[0], one_layer, 0)
        for i, here in enumerate((w_ref, m_ref, v_ref)):
            stores.append(pltpu.make_async_copy(here, out[group * 3 + i], sems.at[group * 4 + i]))
            stores[-1].start()
    for copy in stores:
        copy.wait()


def step_kernel(n, x, dy, wg, wu, wd, *refs):
    (gg_h, gu_h, gd_h, ss, wgu_h, wd_h, st_h, hid_h, a0_h, h1_h, rA) = refs[:11]
    (gg, gu, gd, act, stage, wcomb, wdc, scl, acc, sst, ssr, lb, l2) = refs[11:24]
    (sx, sw, swd, s_stage, shid, sm, ag_loc, ag_s, ag_r, rs_s, rs_r, rs_l, ss_s, ss_r) = refs[24:]
    L, R, FF = wg.shape
    RF, D = wd.shape[1:]
    T = x.shape[0]
    S = math.isqrt(n)
    NC = FF // CH
    NI = L * NC
    NJ = T // TB
    NB = T // TD
    NW = 3
    HW = RF // 2 // NW
    RC = RF // NC
    RB = R + SUB * pl.cdiv(D, CH)
    me, rep = lax.axis_index("dp"), lax.axis_index("rep")
    px, py = me // S, me % S
    par = rep % SLOTS
    one_chunk = wgu_h.at[0, 0, 0]
    partner = {"rep": rep + 1 - 2 * par, "dp": me}
    aT, dyT = act.at[0], act.at[1]
    vmem = pltpu.VMEM

    def at(ix, iy):
        return {"dp": (ix % S) * S + iy % S}

    def send(src, dst, s, r, to):
        pltpu.make_async_remote_copy(src_ref=src, dst_ref=dst, send_sem=s, recv_sem=r, device_id=to, device_id_type=MESH).start()

    def wait(ref, sem):
        pltpu.make_async_copy(ref, ref, sem).wait()

    def cols(c):
        return pl.ds(pl.multiple_of(c * CH, CH), CH)

    def blocks(b, size):
        return pl.ds(pl.multiple_of(b * size, size), size)

    def load_w(i, slot):
        for h in range(HALVES):
            pltpu.make_async_copy(wgu_h.at[h, i // NC, i % NC], wcomb.at[slot, :, :, :, pl.ds(h * CH, CH)], sw.at[slot, h]).start()

    def wait_w(slot):
        for h in range(HALVES):
            wait(one_chunk, sw.at[slot, h])

    def load_wd(l, c, slot):
        return pltpu.make_async_copy(wd_h.at[l, cols(c)], wdc.at[slot], swd.at[slot])

    def item(k):
        return L - 1 - k // NC, NC - 1 - k % NC

    def load_stage(k, j):
        l, c = item(k)
        return pltpu.make_async_copy(st_h.at[l, c, :, blocks(j, TB)], stage.at[j], s_stage.at[j])

    def norm(src, dst):
        def rows(g):
            return pl.ds(g * PACK, PACK)

        total = jnp.zeros((SUB, src.shape[1]), f32)
        for g in range(D // (PACK)):
            wide = src[rows(g), :].astype(f32)
            wide = wide * wide
            total += wide[:SUB] + wide[SUB:]
        scale = lax.rsqrt(jnp.sum(total, axis=0, keepdims=True) / D + 1e-6)
        for g in range(D // (PACK)):
            dst[rows(g), :] = (src[rows(g), :].astype(f32) * scale).astype(bf16)
        return scale

    def forward(hiddenT, w_down, xs, dys, h1s, wl, wdl, sh, sdy):
        def with_down(i):
            return pl.when((i % NC >= NW) & (i % NC % PAIR == 1))

        def rows(d, c):
            return pl.ds(pl.multiple_of(d * RF + par * (RF // 2) + (c - NW) // PAIR * HW, 8), HW)

        def ag1(i):
            l, c = i // NC, i % NC
            p = i % AHEAD
            src, own = wl.at[par, l, :, cols(c)], wgu_h.at[par, l, c, px, py]
            for r in range(1, S):
                send(src, own, ag_s.at[0, p, 0], ag_r.at[0, i, 0], at(px + r * (1 - par), py + r * par))
            pltpu.make_async_copy(src, own, ag_loc.at[p, 0]).start()

            @with_down(i)
            def _():
                src, own = wdl.at[l, par * NW + (c - NW) // PAIR], wd_h.at[l, rows(me, c)]
                for r in range(1, S):
                    send(src, own, ag_s.at[0, p, 1], ag_r.at[0, i, 1], at(px + r * (1 - par), py + r * par))
                pltpu.make_async_copy(src, own, ag_loc.at[p, 1]).start()

        def ag2(i):
            l, c = i // NC, i % NC
            p = i % AHEAD
            for sem in (ag_r.at[0, i, 0], ag_s.at[0, p, 0]):
                wait(wgu_h.at[0, 0, 0, 0, pl.ds(0, S - 1)], sem)
            wait(wgu_h.at[0, 0, 0, 0, 0], ag_loc.at[p, 0])

            @pl.when(par == 0)
            def _():
                w = wgu_h.at[0, l, c, :, py]
                for r in range(1, S):
                    send(w, w, ag_s.at[1, p, 0], ag_r.at[1, i, 0], at(px, py + r))

            @pl.when(par == 1)
            def _():
                w = wgu_h.at[1, l, c, px]
                for r in range(1, S):
                    send(w, w, ag_s.at[1, p, 0], ag_r.at[1, i, 0], at(px + r, py))

            @with_down(i)
            def _():
                for sem in (ag_r.at[0, i, 1], ag_s.at[0, p, 1]):
                    wait(wd_h.at[0, pl.ds(0, (S - 1) * HW)], sem)
                wait(wd_h.at[0, pl.ds(0, HW)], ag_loc.at[p, 1])
                for k in range(S):
                    v = wd_h.at[l, rows((1 - par) * (S * k + py) + par * (S * px + k), c)]
                    for r in range(1, S):
                        send(v, v, ag_s.at[1, p, 1], ag_r.at[1, i, 1], at(px + r * par, py + r * (1 - par)))

        def ag3(i):
            l, c = i // NC, i % NC
            p = i % AHEAD
            for sem in (ag_r.at[1, i, 0], ag_s.at[1, p, 0]):
                wait(wgu_h.at[0, 0, 0, pl.ds(0, S - 1)], sem)
            w = wgu_h.at[par, l, c]
            send(w, w, ag_s.at[2, p, 0], ag_r.at[2, i, 0], partner)

            @with_down(i - 1)
            def _():
                for sem in (ag_r.at[1, i - 1, 1], ag_s.at[1, (i - 1) % AHEAD, 1]):
                    wait(wd_h.at[0, pl.ds(0, S * (S - 1) * HW)], sem)
                for d in range(n):
                    v = wd_h.at[l, rows(d, (i - 1) % NC)]
                    send(v, v, ag_s.at[2, (i - 1) % AHEAD, 1], ag_r.at[2, i - 1, 1], partner)

        def ag4(i):
            for sem in (ag_r.at[2, i, 0], ag_s.at[2, i % AHEAD, 0]):
                wait(one_chunk, sem)

            @with_down(i - 1)
            def _():
                for sem in (ag_r.at[2, i - 1, 1], ag_s.at[2, (i - 1) % AHEAD, 1]):
                    wait(wd_h.at[0, pl.ds(0, n * HW)], sem)

        pltpu.make_async_copy(wg, wl.at[0], sm.at[0]).start()
        pltpu.make_async_copy(wu, wl.at[1], sm.at[1]).start()
        for l in range(L):
            for q in range(RF // HW):
                pltpu.make_async_copy(wd.at[l, pl.ds(q * HW, HW)], wdl.at[l, q], sm.at[2]).start()
        barrier = pltpu.get_barrier_semaphore()
        for r in range(1, n):
            pl.semaphore_signal(barrier, inc=1, device_id={"dp": (me + r) % n}, device_id_type=MESH)
        pl.semaphore_signal(barrier, inc=1, device_id=partner, device_id_type=MESH)

        def fetch(b):
            return pltpu.make_async_copy(x.at[blocks(b, TD)], xs.at[b % SLOTS], sx.at[b % SLOTS])

        def turn(b, _):
            pl.when(b + 1 < NB)(lambda: fetch(b + 1).start())
            fetch(b).wait()
            aT[:, blocks(b, TD)] = xs[b % SLOTS].T
            before = blocks((b + NB - 1) % NB, TD)
            norm(aT.at[:, before], aT.at[:, before])
            return 0

        fetch(0).start()
        wait(wl.at[0], sm.at[0])
        wait(wl.at[1], sm.at[1])
        wait(wdl, sm.at[2])
        pl.semaphore_wait(barrier, n)
        for i in range(3):
            ag1(i)
        lax.fori_loop(0, 3, turn, 0)
        ag2(0)
        ag1(3)
        lax.fori_loop(3, NB - 2, turn, 0)
        ag2(1)
        lax.fori_loop(NB - 2, NB, turn, 0)
        norm(aT.at[:, blocks(NB - 1, TD)], aT.at[:, blocks(NB - 1, TD)])
        acc[...] = jnp.zeros_like(acc)
        ag3(0)
        ag4(0)
        load_w(0, 0)
        ag2(2)
        ag1(4)
        pltpu.make_async_copy(aT, a0_h, sm.at[0]).start()
        ag3(1)

        def load_down(third):
            some = [cols(third * (NC // NW) + i) for i in range(NC // NW)]
            return [pltpu.make_async_copy(wd_h.at[0, rows_], w_down.at[rows_], swd.at[0]) for rows_ in some]

        def start_down(third):
            for copy in load_down(third):
                copy.start()

        def down():
            wait(w_down, swd.at[0])
            wait(aT, sm.at[0])

            def save(b):
                return pltpu.make_async_copy(h1s.at[b % SLOTS], h1_h.at[:, blocks(b, TD)], sh.at[b % SLOTS])

            def normed(b):
                scl[:, blocks(b, TD)] = norm(h1s.at[b % SLOTS], aT.at[:, blocks(b, TD)])

            def block(b, _):
                @pl.when(b + 1 < NB)
                def _():
                    fetch(b + 1).start()

                fetch(b).wait()
                pl.when(b >= 2)(lambda: save(b - 2).wait())
                out = dot(w_down[...], hiddenT[:, blocks(b, TD)], TN).astype(bf16)
                normed((b + NB - 1) % NB)
                h1s[b % SLOTS] = xs[b % SLOTS].T + out
                save(b).start()
                return 0

            lax.fori_loop(0, NB, block, 0)
            normed(NB - 1)
            for b in range(NB - 2, NB):
                save(b).wait()

        def save_hidden(i):
            for part in range(4):
                rows_ = pl.ds(pl.multiple_of(i % NC * CH + part * (CH // 4), CH // 4), CH // 4)
                pltpu.make_async_copy(hiddenT.at[rows_], hid_h.at[i // NC, rows_], shid.at[i % SLOTS]).start()

        def hidden_saved(i):
            wait(hiddenT.at[pl.ds(0, CH)], shid.at[i % SLOTS])

        def part_of_dy(i):
            return i % (T // CH)

        def fetch_dy(i):
            return pltpu.make_async_copy(dy.at[cols(part_of_dy(i))], dys.at[i % SLOTS], sdy.at[i % SLOTS])

        fetch_dy(0).start()

        def chunk(i, _):
            l, c = i // NC, i % NC
            pl.when((c == 0) & (l > 0))(down)
            slot = i % SLOTS
            pl.when(i + 1 < NI)(lambda: fetch_dy(i + 1).start())
            fetch_dy(i).wait()
            wait_w(slot)
            pl.when(i + 3 < NI)(lambda: ag2(i + 3))
            pl.when(i + 5 < NI)(lambda: ag1(i + 5))

            def block(j, _):
                @pl.when((j == NJ - 1) & (i + 1 < NI))
                def _():
                    ag4(i + 1)
                    load_w(i + 1, 1 - slot)

                pl.when((j == NJ - 1) & (i + 2 < NI))(lambda: ag3(i + 2))
                for third in range(NW):
                    pl.when((i == NC - 1) & (j == (third + 1) // PAIR))(lambda: start_down(third))
                pl.when((i == NC - 1) & (j == NJ - 1))(lambda: fetch(0).start())

                @pl.when(i > 0)
                def _():
                    wait(stage.at[j], s_stage.at[j])

                t = blocks(j, TB)
                r = dot(wcomb[slot].reshape(D, WIDE), aT[:, t], TN)
                gate, up = r[:CH], r[CH:]
                sig = 0.5 * jnp.tanh(0.5 * gate) + 0.5
                silu = gate * sig
                stage[j, :CH, :] = silu
                stage[j, CH:, :] = up * (sig + silu * (1.0 - sig))
                hiddenT[cols(c), t] = (silu * up).astype(bf16)
                turned = pl.ds(pl.multiple_of(part_of_dy(i) * CH + j * (CH // NJ), LANES), CH // NJ)
                dyT[:, turned] = dys[slot, blocks(j, CH // NJ), :].T
                pl.when(i + 1 < NI)(lambda: pltpu.make_async_copy(stage.at[j], st_h.at[l, c, :, t], s_stage.at[j]).start())
                return 0

            lax.fori_loop(0, NJ, block, 0)
            pl.when(i >= 2)(lambda: hidden_saved(i - 2))
            save_hidden(i)
            return 0

        lax.fori_loop(0, NI, chunk, 0)
        load_wd(*item(0), 0).start()
        load_w(item(0)[0] * NC + item(0)[1], 0)
        for i in range(NI - SLOTS, NI):
            hidden_saved(i)

    dma = pltpu.SemaphoreType.DMA
    pl.run_scoped(
        forward,
        vmem((FF, T), bf16),
        vmem((FF, D), bf16),
        vmem((SLOTS, TD, D), bf16),
        vmem((SLOTS, CH, D), bf16),
        vmem((SLOTS, D, TD), bf16),
        vmem((SLOTS, L, R, FF), bf16),
        vmem((L, RF // HW, HW, D), bf16),
        dma((SLOTS,)),
        dma((SLOTS,)),
    )

    def backward(daT, big, hid, Fg, Fd, s1, sb, s2, o1, o2, la, sh):
        pieces = [(pl.ds(0, R), pl.ds(0, CH))] + [(pl.ds(R + i * SUB, SUB), pl.ds(0, min(CH, D - i * CH))) for i in range(pl.cdiv(D, CH))]

        def down_piece(i):
            return pl.ds((i - 1) * CH, pieces[i][1].size)

        def places(h, a, b):
            return (a, b) if h == 0 else (b, a)

        def own_sums(p, d, h, i):
            return Fd[p, d, pl.ds(h * SUB, SUB), down_piece(i)] if i else Fg[p, d, :, pl.ds(h * CH, CH)]

        def near(u, a):
            return a + 1 - a % PAIR * PAIR if u == 0 else S - 1 - a

        def far(u, a):
            return near(1 - u, a)

        def rs_send(k):
            l, c = item(k)
            p = k % SLOTS
            for h in range(HALVES):
                a, b = places(h, px, py)
                for u in range(HALVES):
                    src = s1.at[p, h, pl.ds(1 + (a + u) % PAIR, PAIR), pl.ds(u * PAIR, PAIR)]
                    send(src, rA.at[l, c, h, u], rs_s.at[0, p], rs_r.at[k, 0], at(*places(h, near(u, a), b)))

        def rs_pass_b(k):
            p = k % SLOTS

            @pl.when((k >= 2) & (k < NI + 2))
            def _():
                for h in range(HALVES):
                    a, b = places(h, px, py)
                    for u in range(HALVES):
                        src = sb.at[p, h, pl.ds(u * PAIR, PAIR)]
                        send(src, lb.at[(k - 2) % NW, h, u], rs_s.at[1, p], rs_r.at[k - 2, 1], at(*places(h, far(u, a), b)))

        def rs_pass_2(k):
            p = k % SLOTS

            @pl.when((k >= 3) & (k < NI + 3))
            def _():
                for h in range(HALVES):
                    a, b = places(h, px, py)
                    for r in range(1, S):
                        to = at(*places(h, a, b + r))
                        send(s2.at[1 - p, h, (b + r) % S], l2.at[(k - 3) % AHEAD, h, S - 1 - r], rs_s.at[2, 1 - p], rs_r.at[k - 3, 2], to)

        def rs_early(k):
            @pl.when((k >= 2) & (k < NI + 2))
            def _():
                l, c = item(k - 2)
                wait(rA.at[l, c], rs_r.at[k - 2, 0])
                wait(rA.at[l, c], rs_s.at[0, k % SLOTS])
                pltpu.make_async_copy(rA.at[l, c], la, rs_l).start()

        def rs_arrived_a(k):
            pl.when((k >= 2) & (k < NI + 2))(lambda: wait(la, rs_l))

        def rs_arrived(k, stage_of, here):
            q = k - 2 - stage_of

            @pl.when((q >= 0) & (q < NI))
            def _():
                wait(here.at[0], rs_r.at[q, stage_of])
                wait(here.at[0], rs_s.at[stage_of, q % SLOTS])

        def landed(k, lag, slots):
            any_yet = (k + NI + 4 - lag) // (NI + 4)
            return any_yet * ((k + (slots - 1) * lag) % slots) + (1 - any_yet) * (slots - 1)

        def rs_last(k):
            q = (k + NI - 4) % NI
            l, c = item(q)
            landing = landed(k, 4, AHEAD)
            squares = jnp.zeros(TILE, f32)
            for h in range(HALVES):
                for i, piece in enumerate(pieces):
                    total = o2[(q % SLOTS, h) + piece]
                    for j in range(S - 1):
                        total += l2[(landing, h, j) + piece].astype(f32)
                    g = total.astype(bf16)
                    if i:
                        gd[l, pl.ds(pl.multiple_of(c * RC + h * SUB, SUB), SUB), down_piece(i)] = g
                    else:
                        (gg, gu)[h][l, :, cols(c)] = g
                    g = g.astype(f32)
                    g = g * g
                    for a in range(g.shape[0] // SUB):
                        for b in range(g.shape[1] // LANES):
                            squares += g[a * SUB : (a + 1) * SUB, b * LANES : (b + 1) * LANES]
            acc[...] += jnp.where(k >= 4, squares, 0.0)

        def rs_sums_b(k):
            p = (k + 1) % SLOTS
            landing = landed(k, 3, NW)
            for h in range(HALVES):
                a, b = places(h, px, py)
                for i, piece in enumerate(pieces):
                    for s in range(S):
                        total = o1[(p, h, s) + piece] + lb[(landing, h, s // PAIR, s % PAIR) + piece].astype(f32)
                        s2[(p, h, s) + piece] = total.astype(bf16)
                        own = jnp.where(b == s, total, own) if s else total
                    o2[(p, h) + piece] = own

        def rs_sums_a(k):
            p = k % SLOTS
            for h in range(HALVES):
                a, b = places(h, px, py)
                for i, piece in enumerate(pieces):
                    for s in range(S):
                        u = s // PAIR
                        ours = (a + 1 + u) % PAIR
                        for keep_it, first, index in ((True, a, ours), (False, far(u, a), 1 - ours)):
                            ix, iy = places(h, first, s)
                            total = own_sums(p, ix * S + iy, h, i) + la[(h, u, index, s % PAIR) + piece].astype(f32)
                            if keep_it:
                                o1[(p, h, s) + piece] = total
                            else:
                                sb[(p, h, s) + piece] = total.astype(bf16)

        def load_hidden(k):
            l, c = item(k)
            for d in range(n):
                rows = hid_h.at[l, pl.ds(pl.multiple_of(d * RF + c * RC, 8), RC)]
                pltpu.make_async_copy(rows, hid.at[pl.ds(d * RC, RC)], shid.at[0]).start()

        def at_rows(slot, row, size):
            return pl.ds(row % CH, size), pl.ds(pl.multiple_of(slot * (T // 2) + row // CH * TD, TD), TD)

        def each_h(b, do):
            size = LANES // 2
            for row in range(0, D, size):
                do(pltpu.make_async_copy(h1_h.at[pl.ds(row, size), blocks(b, TD)], hid.at[at_rows(b % SLOTS, row, size)], sh.at[b % SLOTS]))

        def through_norm():
            def block(b, _):
                t = blocks(b, TD)
                pl.when((b > 0) & (b + 1 < NB))(lambda: each_h(b + 1, lambda copy: copy.start()))
                wait(h1_h.at[:, t], sh.at[b % SLOTS])

                def both(g):
                    rows = pl.ds(g, PACK)
                    return daT[rows, t].astype(bf16).astype(f32), hid[at_rows(b % SLOTS, g, PACK)].astype(f32)

                along = jnp.zeros((SUB, TD), f32)
                for g in range(0, D, PACK):
                    da, wide = both(g)
                    wide = da * wide
                    along += wide[:SUB] + wide[SUB:]
                scale = scl[:, t]
                along = jnp.sum(along, axis=0, keepdims=True) * (scale * scale * scale) * (-1 / D)
                for g in range(0, D, PACK):
                    da, wide = both(g)
                    dyT[pl.ds(g, PACK), t] += (da * scale + wide * along).astype(bf16)
                return 0

            lax.fori_loop(0, NB, block, 0)
            load_hidden(NC)

        load_hidden(0)

        def one(k, _):
            l, c = item(k)
            slot = k % SLOTS

            @pl.when(k + 1 < NI)
            def _():
                load_wd(*item(k + 1), 1 - slot).start()

            @pl.when(k == NC)
            def _():
                through_norm()
                wait(aT, sm.at[0])

            @pl.when(k + 1 < NC)
            def _():
                load_w(item(k + 1)[0] * NC + item(k + 1)[1], 1 - slot)

            rs_early(k)
            load_wd(l, c, slot).wait()

            @pl.when(k > 0)
            def _():
                for j in range(NJ):
                    load_stage(k, j).wait()

            dh = dot(wdc[slot], dyT[...])
            for j in range(NJ):
                t = slice(j * TB, (j + 1) * TB)
                part = dh[:, t].astype(bf16).astype(f32)
                big[:CH, t] = (part * stage[j, CH:, :]).astype(bf16)
                big[CH:, t] = (part * stage[j, :CH, :]).astype(bf16)

            @pl.when(k + 1 < NI)
            def _():
                for j in range(NJ):
                    load_stage(k + 1, j).start()

            rs_arrived_a(k)
            rs_arrived(k, 1, lb)
            rs_sums_b(k)
            rs_sums_a(k)

            def to_send(d, h):
                first, second = places(h, d // S, d % S)
                return slot, h, (first + S - (px, py)[h]) % S, second

            wide = dot(aT[...], big[...], NT)
            for d in range(n):
                block = wide[d * R : (d + 1) * R]
                Fg[slot, d] = block
                for h in range(HALVES):
                    s1[to_send(d, h) + pieces[0]] = block[:, h * CH : (h + 1) * CH].astype(bf16)
            rs_pass_b(k)
            pl.when(k == NC - 1)(lambda: pltpu.make_async_copy(a0_h, aT, sm.at[0]).start())
            wait(hid, shid.at[0])
            rs_arrived(k, 2, l2)

            @pl.when(k < NI)
            def _():
                rs_last(k)
                down = dot(dyT[...], hid[...], NT).T
                for d in range(n):
                    block = down[d * RC : (d + 1) * RC]
                    Fd[slot, d] = block
                    for h in range(HALVES):
                        for i in range(1, len(pieces)):
                            columns = down_piece(i)
                            some = block[h * SUB : (h + 1) * SUB, columns.start : columns.start + columns.size]
                            s1[to_send(d, h) + pieces[i]] = some.astype(bf16)

            rs_pass_2(k)
            rs_send(k)
            pl.when((k + 1 < NI) & (k + 1 != NC))(lambda: load_hidden(k + 1))

            @pl.when(k + 1 == NC)
            def _():
                for b in range(2):
                    each_h(b, lambda copy: copy.start())


            def into(first):
                wait_w(slot)
                da = dot(wcomb[slot].reshape(D, WIDE), big[...])
                daT[...] = da if first else daT[...] + da

            pl.when(k == 0)(lambda: into(True))
            pl.when((k > 0) & (k < NC))(lambda: into(False))
            return 0

        lax.fori_loop(0, NI, one, 0)

        def rest(k, _):
            rs_early(k)
            rs_arrived_a(k)
            rs_sums_a(k)
            rs_pass_b(k)
            rs_arrived(k, 1, lb)
            rs_sums_b(k)
            rs_pass_2(k)
            rs_arrived(k, 2, l2)
            rs_last(k)
            return 0

        lax.fori_loop(NI, NI + 4, rest, 0)

    pl.run_scoped(
        backward,
        vmem((D, T), f32),
        vmem((WIDE, T), bf16),
        vmem((n * RC, T), bf16),
        vmem((SLOTS, n, R, WIDE), f32),
        vmem((SLOTS, n, RC, D), f32),
        vmem((SLOTS, HALVES, S, S, RB, CH), bf16),
        vmem((SLOTS, HALVES, S, RB, CH), bf16),
        vmem((SLOTS, HALVES, S, RB, CH), bf16),
        vmem((SLOTS, HALVES, S, RB, CH), f32),
        vmem((SLOTS, HALVES, RB, CH), f32),
        vmem(rA.shape[2:], bf16),
        dma((SLOTS,)),
    )

    results = [pltpu.make_async_copy(here, to, sm.at[i]) for i, (here, to) in enumerate(((gg, gg_h), (gu, gu_h), (gd, gd_h)))]
    for copy in results:
        copy.start()
    sst[...] = acc[...]
    ssr[me] = acc[...]
    for r in range(1, n):
        send(sst, ssr.at[me], ss_s, ss_r, {"dp": (me + r) % n})
    wait(ssr.at[pl.ds(0, n - 1)], ss_r)
    wait(ssr.at[pl.ds(0, n - 1)], ss_s)
    total = ssr[0]
    for d in range(1, n):
        total += ssr[d]
    ss[...] = total
    for copy in results:
        copy.wait()


def solution(mesh):
    n = mesh.shape["dp"]
    S = math.isqrt(n)

    def step(x, dy, *arrays):
        weights, m, v = (arrays[i : i + 3] for i in (0, 3, 6))
        L, R, FF = weights[0].shape
        RF, D = weights[2].shape[1:]
        T = x.shape[1]
        NC = FF // CH
        RB = R + SUB * pl.cdiv(D, CH)
        NJ = T // TB
        sds = jax.ShapeDtypeStruct
        vmem, dma = pltpu.VMEM, pltpu.SemaphoreType.DMA
        outs = [
            (sds((L, R, FF), bf16), pl.ANY),
            (sds((L, R, FF), bf16), pl.ANY),
            (sds((L, RF, D), bf16), pl.ANY),
            (sds(TILE, f32), pltpu.VMEM),
            (sds((2, L, NC, S, S, R, CH), bf16), pl.ANY),
            (sds((L, FF, D), bf16), pl.ANY),
            (sds((L, NC, WIDE, T), f32), pl.ANY),
            (sds((L, FF, T), bf16), pl.ANY),
            (sds((D, T), bf16), pl.ANY),
            (sds((D, T), bf16), pl.ANY),
            (sds((L, NC, HALVES, HALVES, PAIR, PAIR, RB, CH), bf16), pl.ANY),
        ]
        scratch = [
            vmem((L, R, FF), bf16),
            vmem((L, R, FF), bf16),
            vmem((L, RF, D), bf16),
            vmem((SLOTS, D, T), bf16),
            vmem((NJ, WIDE, TB), f32),
            vmem((SLOTS, S, S, R, WIDE), bf16),
            vmem((SLOTS, CH, D), bf16),
            vmem((1, T), f32),
            vmem(TILE, f32),
            vmem(TILE, f32),
            vmem((n,) + TILE, f32),
            vmem((3, HALVES, HALVES, PAIR, RB, CH), bf16),
            vmem((AHEAD, HALVES, S - 1, RB, CH), bf16),
            dma((SLOTS,)),
            dma((2, 2)),
            dma((SLOTS,)),
            dma((NJ,)),
            dma((SLOTS,)),
            dma((3,)),
            dma((AHEAD, 2)),
            dma((3, AHEAD, 2)),
            dma((3, L * NC, 2)),
            dma((3, SLOTS)),
            dma((L * NC, 3)),
            dma(()),
            dma(()),
            dma(()),
        ]
        flops = 15 * 2 * T * D * FF
        done = pl.pallas_call(
            lambda *refs: step_kernel(n, *refs),
            in_specs=[pl.BlockSpec(memory_space=pl.ANY)] * 5,
            out_specs=[pl.BlockSpec(memory_space=space) for _, space in outs],
            out_shape=[shape for shape, _ in outs],
            scratch_shapes=scratch,
            compiler_params=pltpu.CompilerParams(
                collective_id=0,
                has_side_effects=True,
                vmem_limit_bytes=VMEM_BYTES,
            ),
            cost_estimate=pl.CostEstimate(flops=flops, bytes_accessed=400 << 20, transcendentals=0),
            name="train_step",
        )(x[0], dy[0], *weights)
        gradients = done[:3]
        count = n * sum(g.size for g in gradients)
        old = [array for g, w, m_, v_ in zip(gradients, weights, m, v, strict=True) for array in (g, w, m_, v_)]
        new = pl.pallas_call(
            lambda *refs: adamw_kernel(count, *refs),
            in_specs=[pl.BlockSpec(memory_space=pltpu.VMEM)] + [pl.BlockSpec(memory_space=pl.ANY)] * len(old),
            out_specs=[pl.BlockSpec(memory_space=pl.ANY)] * (len(weights) * 3),
            out_shape=[sds(a.shape, a.dtype) for w, m_, v_ in zip(weights, m, v, strict=True) for a in (w, m_, v_)],
            scratch_shapes=[vmem(a.shape, a.dtype) for a in old] + [dma((len(old),))],
            compiler_params=pltpu.CompilerParams(vmem_limit_bytes=VMEM_BYTES),
            name="adamw",
        )(done[3], *old)
        return tuple(new[i] for which in range(3) for i in range(which, len(new), 3))

    states, cut = P(("rep", "dp"), None, None), P(None, "dp", None)
    return jax.shard_map(
        step,
        mesh=mesh,
        in_specs=(states, states) + (cut,) * 9,
        out_specs=(P("rep", "dp", None),) * 9,
        check_vma=False,
    )
```

```python
import math

import jax
import jax.numpy as jnp
from jax import lax
from jax.experimental import pallas as pl
from jax.experimental.pallas import tpu as pltpu
from jax.sharding import PartitionSpec as P

bf16, f32 = jnp.bfloat16, jnp.float32
MESH = pl.DeviceIdType.MESH
CH = 256
TB = 2048
TD = 2 * CH
TILE = SUB, LANES = 8, 128
PACK = 2 * SUB
WIDE = 2 * CH
VMEM_BYTES = 67043328
AHEAD = 4
SLOTS = HALVES = KINDS = PAIR = 2
NN = (((1,), (0,)), ((), ()))
NT = (((1,), (1,)), ((), ()))
TN = (((0,), (0,)), ((), ()))


def dot(a, b, dims=NN):
    return lax.dot_general(a, b, dims, preferred_element_type=f32)


def adamw_kernel(count, squares, *refs):
    groups = len(refs) // 11
    arrays, out, held, sems = refs[: groups * 4], refs[groups * 4 : groups * 7], refs[groups * 7 : -1], refs[-1]
    for i, (array, here) in enumerate(zip(arrays, held, strict=True)):
        pltpu.make_async_copy(array, here, sems.at[i]).start()
    total = jnp.sum(squares[...], keepdims=True)
    factor = jnp.minimum(1.0, 0.5 * lax.rsqrt(total / count + 1e-30))
    stores = []
    for group in range(groups):
        g_ref, w_ref, m_ref, v_ref = held[group * 4 : group * 4 + 4]
        for i in range(group * 4, group * 4 + 4):
            pltpu.make_async_copy(arrays[i], held[i], sems.at[i]).wait()
        def one_layer(at, _):
            g = g_ref[at].astype(f32) * factor
            w = w_ref[at].astype(f32)
            m = 0.9 * m_ref[at] + 0.1 * g
            v = 0.95 * v_ref[at] + 0.05 * g * g
            step = m * lax.rsqrt(v + 1e-8) + 0.1 * w
            w_ref[at] = (w - 0.02 * step).astype(bf16)
            m_ref[at] = m
            v_ref[at] = v
            return 0

        lax.fori_loop(0, g_ref.shape[0], one_layer, 0)
        for i, here in enumerate((w_ref, m_ref, v_ref)):
            stores.append(pltpu.make_async_copy(here, out[group * 3 + i], sems.at[group * 4 + i]))
            stores[-1].start()
    for copy in stores:
        copy.wait()


def step_kernel(n, x, dy, wg, wu, wd, *refs):
    (gg_h, gu_h, gd_h, ss, wgu_h, wd_h, st_h, hid_h, a0_h, h1_h, rA) = refs[:11]
    (gg, gu, gd, act, stage, wcomb, wdc, scl, acc, sst, ssr, lb, l2) = refs[11:24]
    (sx, sw, swd, s_stage, shid, sm, ag_loc, ag_s, ag_r, rs_s, rs_r, rs_l, ss_s, ss_r) = refs[24:]
    L, R, FF = wg.shape
    RF, D = wd.shape[1:]
    T = x.shape[0]
    S = math.isqrt(n)
    NC = FF // CH
    NI = L * NC
    NJ = T // TB
    NB = T // TD
    NW = 3
    HW = RF // 2 // NW
    RC = RF // NC
    RB = R + SUB * pl.cdiv(D, CH)
    me, rep = lax.axis_index("dp"), lax.axis_index("rep")
    px, py = me // S, me % S
    par = rep % SLOTS
    one_chunk = wgu_h.at[0, 0, 0]
    partner = {"rep": rep + 1 - 2 * par, "dp": me}
    aT, dyT = act.at[0], act.at[1]
    vmem = pltpu.VMEM

    def at(ix, iy):
        return {"dp": (ix % S) * S + iy % S}

    def send(src, dst, s, r, to):
        pltpu.make_async_remote_copy(src_ref=src, dst_ref=dst, send_sem=s, recv_sem=r, device_id=to, device_id_type=MESH).start()

    def wait(ref, sem):
        pltpu.make_async_copy(ref, ref, sem).wait()

    def cols(c):
        return pl.ds(pl.multiple_of(c * CH, CH), CH)

    def blocks(b, size):
        return pl.ds(pl.multiple_of(b * size, size), size)

    def load_w(i, slot):
        for h in range(HALVES):
            pltpu.make_async_copy(wgu_h.at[h, i // NC, i % NC], wcomb.at[slot, :, :, :, pl.ds(h * CH, CH)], sw.at[slot, h]).start()

    def wait_w(slot):
        for h in range(HALVES):
            wait(one_chunk, sw.at[slot, h])

    def load_wd(l, c, slot):
        return pltpu.make_async_copy(wd_h.at[l, cols(c)], wdc.at[slot], swd.at[slot])

    def item(k):
        return L - 1 - k // NC, NC - 1 - k % NC

    def load_stage(k, j):
        l, c = item(k)
        return pltpu.make_async_copy(st_h.at[l, c, :, blocks(j, TB)], stage.at[j], s_stage.at[j])

    def norm(src, dst):
        def rows(g):
            return pl.ds(g * PACK, PACK)

        total = jnp.zeros((SUB, src.shape[1]), f32)
        for g in range(D // (PACK)):
            wide = src[rows(g), :].astype(f32)
            wide = wide * wide
            total += wide[:SUB] + wide[SUB:]
        scale = lax.rsqrt(jnp.sum(total, axis=0, keepdims=True) / D + 1e-6)
        for g in range(D // (PACK)):
            dst[rows(g), :] = (src[rows(g), :].astype(f32) * scale).astype(bf16)
        return scale

    def forward(hiddenT, w_down, xs, dys, h1s, wl, wdl, sh, sdy):
        def with_down(i):
            return pl.when((i % NC >= NW) & (i % NC % PAIR == 1))

        def rows(d, c):
            return pl.ds(pl.multiple_of(d * RF + par * (RF // 2) + (c - NW) // PAIR * HW, 8), HW)

        def ag1(i):
            l, c = i // NC, i % NC
            p = i % AHEAD
            src, own = wl.at[par, l, :, cols(c)], wgu_h.at[par, l, c, px, py]
            for r in range(1, S):
                send(src, own, ag_s.at[0, p, 0], ag_r.at[0, i, 0], at(px + r * (1 - par), py + r * par))
            pltpu.make_async_copy(src, own, ag_loc.at[p, 0]).start()

            @with_down(i)
            def _():
                src, own = wdl.at[l, par * NW + (c - NW) // PAIR], wd_h.at[l, rows(me, c)]
                for r in range(1, S):
                    send(src, own, ag_s.at[0, p, 1], ag_r.at[0, i, 1], at(px + r * (1 - par), py + r * par))
                pltpu.make_async_copy(src, own, ag_loc.at[p, 1]).start()

        def ag2(i):
            l, c = i // NC, i % NC
            p = i % AHEAD
            for sem in (ag_r.at[0, i, 0], ag_s.at[0, p, 0]):
                wait(wgu_h.at[0, 0, 0, 0, pl.ds(0, S - 1)], sem)
            wait(wgu_h.at[0, 0, 0, 0, 0], ag_loc.at[p, 0])

            @pl.when(par == 0)
            def _():
                w = wgu_h.at[0, l, c, :, py]
                for r in range(1, S):
                    send(w, w, ag_s.at[1, p, 0], ag_r.at[1, i, 0], at(px, py + r))

            @pl.when(par == 1)
            def _():
                w = wgu_h.at[1, l, c, px]
                for r in range(1, S):
                    send(w, w, ag_s.at[1, p, 0], ag_r.at[1, i, 0], at(px + r, py))

            @with_down(i)
            def _():
                for sem in (ag_r.at[0, i, 1], ag_s.at[0, p, 1]):
                    wait(wd_h.at[0, pl.ds(0, (S - 1) * HW)], sem)
                wait(wd_h.at[0, pl.ds(0, HW)], ag_loc.at[p, 1])
                for k in range(S):
                    v = wd_h.at[l, rows((1 - par) * (S * k + py) + par * (S * px + k), c)]
                    for r in range(1, S):
                        send(v, v, ag_s.at[1, p, 1], ag_r.at[1, i, 1], at(px + r * par, py + r * (1 - par)))

        def ag3(i):
            l, c = i // NC, i % NC
            p = i % AHEAD
            for sem in (ag_r.at[1, i, 0], ag_s.at[1, p, 0]):
                wait(wgu_h.at[0, 0, 0, pl.ds(0, S - 1)], sem)
            w = wgu_h.at[par, l, c]
            send(w, w, ag_s.at[2, p, 0], ag_r.at[2, i, 0], partner)

            @with_down(i - 1)
            def _():
                for sem in (ag_r.at[1, i - 1, 1], ag_s.at[1, (i - 1) % AHEAD, 1]):
                    wait(wd_h.at[0, pl.ds(0, S * (S - 1) * HW)], sem)
                for d in range(n):
                    v = wd_h.at[l, rows(d, (i - 1) % NC)]
                    send(v, v, ag_s.at[2, (i - 1) % AHEAD, 1], ag_r.at[2, i - 1, 1], partner)

        def ag4(i):
            for sem in (ag_r.at[2, i, 0], ag_s.at[2, i % AHEAD, 0]):
                wait(one_chunk, sem)

            @with_down(i - 1)
            def _():
                for sem in (ag_r.at[2, i - 1, 1], ag_s.at[2, (i - 1) % AHEAD, 1]):
                    wait(wd_h.at[0, pl.ds(0, n * HW)], sem)

        pltpu.make_async_copy(wg, wl.at[0], sm.at[0]).start()
        pltpu.make_async_copy(wu, wl.at[1], sm.at[1]).start()
        for l in range(L):
            for q in range(RF // HW):
                pltpu.make_async_copy(wd.at[l, pl.ds(q * HW, HW)], wdl.at[l, q], sm.at[2]).start()
        barrier = pltpu.get_barrier_semaphore()
        for r in range(1, n):
            pl.semaphore_signal(barrier, inc=1, device_id={"dp": (me + r) % n}, device_id_type=MESH)
        pl.semaphore_signal(barrier, inc=1, device_id=partner, device_id_type=MESH)

        def fetch(b):
            return pltpu.make_async_copy(x.at[blocks(b, TD)], xs.at[b % SLOTS], sx.at[b % SLOTS])

        def turn(b, _):
            pl.when(b + 1 < NB)(lambda: fetch(b + 1).start())
            fetch(b).wait()
            aT[:, blocks(b, TD)] = xs[b % SLOTS].T
            before = blocks((b + NB - 1) % NB, TD)
            norm(aT.at[:, before], aT.at[:, before])
            return 0

        def part_of_dy(i):
            return i % (T // CH)

        def fetch_dy(i):
            return pltpu.make_async_copy(dy.at[cols(part_of_dy(i))], dys.at[i % SLOTS], sdy.at[i % SLOTS])

        fetch(0).start()
        fetch_dy(0).start()
        wait(wl.at[0], sm.at[0])
        wait(wl.at[1], sm.at[1])
        wait(wdl, sm.at[2])
        pl.semaphore_wait(barrier, n)
        for i in range(3):
            ag1(i)
        lax.fori_loop(0, 3, turn, 0)
        ag2(0)
        ag1(3)
        lax.fori_loop(3, NB - 2, turn, 0)
        ag2(1)
        lax.fori_loop(NB - 2, NB, turn, 0)
        ag2(2)
        ag1(4)
        norm(aT.at[:, blocks(NB - 1, TD)], aT.at[:, blocks(NB - 1, TD)])
        acc[...] = jnp.zeros_like(acc)
        ag3(0)
        ag4(0)
        load_w(0, 0)
        pltpu.make_async_copy(aT, a0_h, sm.at[0]).start()
        ag3(1)

        def load_down(third):
            some = [cols(third * (NC // NW) + i) for i in range(NC // NW)]
            return [pltpu.make_async_copy(wd_h.at[0, rows_], w_down.at[rows_], swd.at[0]) for rows_ in some]

        def start_down(third):
            for copy in load_down(third):
                copy.start()

        def down():
            wait(w_down, swd.at[0])
            wait(aT, sm.at[0])

            def save(b):
                return pltpu.make_async_copy(h1s.at[b % SLOTS], h1_h.at[:, blocks(b, TD)], sh.at[b % SLOTS])

            def normed(b):
                scl[:, blocks(b, TD)] = norm(h1s.at[b % SLOTS], aT.at[:, blocks(b, TD)])

            def block(b, _):
                @pl.when(b + 1 < NB)
                def _():
                    fetch(b + 1).start()

                fetch(b).wait()
                pl.when(b >= 2)(lambda: save(b - 2).wait())
                out = dot(w_down[...], hiddenT[:, blocks(b, TD)], TN).astype(bf16)
                normed((b + NB - 1) % NB)
                h1s[b % SLOTS] = xs[b % SLOTS].T + out
                save(b).start()
                return 0

            lax.fori_loop(0, NB, block, 0)
            normed(NB - 1)
            for b in range(NB - 2, NB):
                save(b).wait()

        def save_hidden(i):
            for part in range(4):
                rows_ = pl.ds(pl.multiple_of(i % NC * CH + part * (CH // 4), CH // 4), CH // 4)
                pltpu.make_async_copy(hiddenT.at[rows_], hid_h.at[i // NC, rows_], shid.at[i % SLOTS]).start()

        def hidden_saved(i):
            wait(hiddenT.at[pl.ds(0, CH)], shid.at[i % SLOTS])

        def chunk(i, _):
            l, c = i // NC, i % NC
            pl.when((c == 0) & (l > 0))(down)
            slot = i % SLOTS
            pl.when(i + 1 < NI)(lambda: fetch_dy(i + 1).start())
            fetch_dy(i).wait()
            wait_w(slot)
            pl.when(i + 3 < NI)(lambda: ag2(i + 3))
            pl.when(i + 5 < NI)(lambda: ag1(i + 5))

            def block(j, _):
                @pl.when((j == NJ - 1) & (i + 1 < NI))
                def _():
                    ag4(i + 1)
                    load_w(i + 1, 1 - slot)

                pl.when((j == NJ - 1) & (i + 2 < NI))(lambda: ag3(i + 2))
                for third in range(NW):
                    pl.when((i == NC - 1) & (j == (third + 1) // PAIR))(lambda: start_down(third))
                pl.when((i == NC - 1) & (j == NJ - 1))(lambda: fetch(0).start())

                @pl.when(i > 0)
                def _():
                    wait(stage.at[j], s_stage.at[j])

                t = blocks(j, TB)
                r = dot(wcomb[slot].reshape(D, WIDE), aT[:, t], TN)
                gate, up = r[:CH], r[CH:]
                sig = 0.5 * jnp.tanh(0.5 * gate) + 0.5
                silu = gate * sig
                stage[j, :CH, :] = silu
                stage[j, CH:, :] = up * (sig + silu * (1.0 - sig))
                hiddenT[cols(c), t] = (silu * up).astype(bf16)
                turned = pl.ds(pl.multiple_of(part_of_dy(i) * CH + j * (CH // NJ), LANES), CH // NJ)
                dyT[:, turned] = dys[slot, blocks(j, CH // NJ), :].T
                pl.when(i + 1 < NI)(lambda: pltpu.make_async_copy(stage.at[j], st_h.at[l, c, :, t], s_stage.at[j]).start())
                return 0

            lax.fori_loop(0, NJ, block, 0)
            pl.when(i >= 2)(lambda: hidden_saved(i - 2))
            save_hidden(i)
            return 0

        lax.fori_loop(0, NI, chunk, 0)
        load_wd(*item(0), 0).start()
        load_w(item(0)[0] * NC + item(0)[1], 0)
        for i in range(NI - SLOTS, NI):
            hidden_saved(i)

    dma = pltpu.SemaphoreType.DMA
    pl.run_scoped(
        forward,
        vmem((FF, T), bf16),
        vmem((FF, D), bf16),
        vmem((SLOTS, TD, D), bf16),
        vmem((SLOTS, CH, D), bf16),
        vmem((SLOTS, D, TD), bf16),
        vmem((SLOTS, L, R, FF), bf16),
        vmem((L, RF // HW, HW, D), bf16),
        dma((SLOTS,)),
        dma((SLOTS,)),
    )

    def backward(daT, big, hid, Fg, Fd, s1, sb, s2, o1, o2, la, sh):
        pieces = [(pl.ds(0, R), pl.ds(0, CH))] + [(pl.ds(R + i * SUB, SUB), pl.ds(0, min(CH, D - i * CH))) for i in range(pl.cdiv(D, CH))]

        def down_piece(i):
            return pl.ds((i - 1) * CH, pieces[i][1].size)

        def places(h, a, b):
            return (a, b) if h == 0 else (b, a)

        def own_sums(p, d, h, i):
            return Fd[p, d, pl.ds(h * SUB, SUB), down_piece(i)] if i else Fg[p, d, :, pl.ds(h * CH, CH)]

        def near(u, a):
            return a + 1 - a % PAIR * PAIR if u == 0 else S - 1 - a

        def far(u, a):
            return near(1 - u, a)

        def rs_send(k):
            l, c = item(k)
            p = k % SLOTS
            for h in range(HALVES):
                a, b = places(h, px, py)
                for u in range(HALVES):
                    src = s1.at[p, h, pl.ds(1 + (a + u) % PAIR, PAIR), pl.ds(u * PAIR, PAIR)]
                    send(src, rA.at[l, c, h, u], rs_s.at[0, p], rs_r.at[k, 0], at(*places(h, near(u, a), b)))

        def rs_pass_b(k):
            p = k % SLOTS

            @pl.when((k >= 2) & (k < NI + 2))
            def _():
                for h in range(HALVES):
                    a, b = places(h, px, py)
                    for u in range(HALVES):
                        src = sb.at[p, h, pl.ds(u * PAIR, PAIR)]
                        send(src, lb.at[(k - 2) % NW, h, u], rs_s.at[1, p], rs_r.at[k - 2, 1], at(*places(h, far(u, a), b)))

        def rs_pass_2(k):
            p = k % SLOTS

            @pl.when((k >= 3) & (k < NI + 3))
            def _():
                for h in range(HALVES):
                    a, b = places(h, px, py)
                    for r in range(1, S):
                        to = at(*places(h, a, b + r))
                        send(s2.at[1 - p, h, (b + r) % S], l2.at[(k - 3) % AHEAD, h, S - 1 - r], rs_s.at[2, 1 - p], rs_r.at[k - 3, 2], to)

        def rs_early(k):
            @pl.when((k >= 2) & (k < NI + 2))
            def _():
                l, c = item(k - 2)
                wait(rA.at[l, c], rs_r.at[k - 2, 0])
                wait(rA.at[l, c], rs_s.at[0, k % SLOTS])
                pltpu.make_async_copy(rA.at[l, c], la, rs_l).start()

        def rs_arrived_a(k):
            pl.when((k >= 2) & (k < NI + 2))(lambda: wait(la, rs_l))

        def rs_arrived(k, stage_of, here):
            q = k - 2 - stage_of

            @pl.when((q >= 0) & (q < NI))
            def _():
                wait(here.at[0], rs_r.at[q, stage_of])
                wait(here.at[0], rs_s.at[stage_of, q % SLOTS])

        def landed(k, lag, slots):
            any_yet = (k + NI + 4 - lag) // (NI + 4)
            return any_yet * ((k + (slots - 1) * lag) % slots) + (1 - any_yet) * (slots - 1)

        def rs_last(k):
            q = (k + NI - 4) % NI
            l, c = item(q)
            landing = landed(k, 4, AHEAD)
            squares = jnp.zeros(TILE, f32)
            for h in range(HALVES):
                for i, piece in enumerate(pieces):
                    total = o2[(q % SLOTS, h) + piece]
                    for j in range(S - 1):
                        total += l2[(landing, h, j) + piece].astype(f32)
                    g = total.astype(bf16)
                    if i:
                        gd[l, pl.ds(pl.multiple_of(c * RC + h * SUB, SUB), SUB), down_piece(i)] = g
                    else:
                        (gg, gu)[h][l, :, cols(c)] = g
                    g = g.astype(f32)
                    g = g * g
                    for a in range(g.shape[0] // SUB):
                        for b in range(g.shape[1] // LANES):
                            squares += g[a * SUB : (a + 1) * SUB, b * LANES : (b + 1) * LANES]
            acc[...] += jnp.where(k >= 4, squares, 0.0)

        def rs_sums_b(k):
            p = (k + 1) % SLOTS
            landing = landed(k, 3, NW)
            for h in range(HALVES):
                a, b = places(h, px, py)
                for i, piece in enumerate(pieces):
                    for s in range(S):
                        total = o1[(p, h, s) + piece] + lb[(landing, h, s // PAIR, s % PAIR) + piece].astype(f32)
                        s2[(p, h, s) + piece] = total.astype(bf16)
                        own = jnp.where(b == s, total, own) if s else total
                    o2[(p, h) + piece] = own

        def rs_sums_a(k):
            p = k % SLOTS
            for h in range(HALVES):
                a, b = places(h, px, py)
                for i, piece in enumerate(pieces):
                    for s in range(S):
                        u = s // PAIR
                        ours = (a + 1 + u) % PAIR
                        for keep_it, first, index in ((True, a, ours), (False, far(u, a), 1 - ours)):
                            ix, iy = places(h, first, s)
                            total = own_sums(p, ix * S + iy, h, i) + la[(h, u, index, s % PAIR) + piece].astype(f32)
                            if keep_it:
                                o1[(p, h, s) + piece] = total
                            else:
                                sb[(p, h, s) + piece] = total.astype(bf16)

        def load_hidden(k):
            l, c = item(k)
            for d in range(n):
                rows = hid_h.at[l, pl.ds(pl.multiple_of(d * RF + c * RC, 8), RC)]
                pltpu.make_async_copy(rows, hid.at[pl.ds(d * RC, RC)], shid.at[0]).start()

        def at_rows(slot, row, size):
            return pl.ds(row % CH, size), pl.ds(pl.multiple_of(slot * (T // 2) + row // CH * TD, TD), TD)

        def each_h(b, do):
            size = LANES // 2
            for row in range(0, D, size):
                do(pltpu.make_async_copy(h1_h.at[pl.ds(row, size), blocks(b, TD)], hid.at[at_rows(b % SLOTS, row, size)], sh.at[b % SLOTS]))

        def through_norm():
            def block(b, _):
                t = blocks(b, TD)
                pl.when((b > 0) & (b + 1 < NB))(lambda: each_h(b + 1, lambda copy: copy.start()))
                wait(h1_h.at[:, t], sh.at[b % SLOTS])

                def both(g):
                    rows = pl.ds(g, PACK)
                    return daT[rows, t], hid[at_rows(b % SLOTS, g, PACK)].astype(f32)

                along = jnp.zeros((SUB, TD), f32)
                for g in range(0, D, PACK):
                    da, wide = both(g)
                    wide = da * wide
                    along += wide[:SUB] + wide[SUB:]
                scale = scl[:, t]
                along = jnp.sum(along, axis=0, keepdims=True) * (scale * scale * scale) * (-1 / D)
                for g in range(0, D, PACK):
                    da, wide = both(g)
                    dyT[pl.ds(g, PACK), t] += (da * scale + wide * along).astype(bf16)
                return 0

            lax.fori_loop(0, NB, block, 0)
            load_hidden(NC)

        load_hidden(0)

        def one(k, _):
            l, c = item(k)
            slot = k % SLOTS

            @pl.when(k + 1 < NI)
            def _():
                load_wd(*item(k + 1), 1 - slot).start()

            @pl.when(k == NC)
            def _():
                through_norm()
                wait(aT, sm.at[0])

            @pl.when(k + 1 < NC)
            def _():
                load_w(item(k + 1)[0] * NC + item(k + 1)[1], 1 - slot)

            rs_early(k)
            load_wd(l, c, slot).wait()

            @pl.when(k > 0)
            def _():
                for j in range(NJ):
                    load_stage(k, j).wait()

            dh = dot(wdc[slot], dyT[...])
            for j in range(NJ):
                t = slice(j * TB, (j + 1) * TB)
                part = dh[:, t].astype(bf16).astype(f32)
                big[:CH, t] = (part * stage[j, CH:, :]).astype(bf16)
                big[CH:, t] = (part * stage[j, :CH, :]).astype(bf16)

            @pl.when(k + 1 < NI)
            def _():
                for j in range(NJ):
                    load_stage(k + 1, j).start()

            rs_arrived_a(k)
            rs_arrived(k, 1, lb)
            rs_sums_b(k)
            rs_sums_a(k)

            def to_send(d, h):
                first, second = places(h, d // S, d % S)
                return slot, h, (first + S - (px, py)[h]) % S, second

            wide = dot(aT[...], big[...], NT)
            for d in range(n):
                block = wide[d * R : (d + 1) * R]
                Fg[slot, d] = block
                for h in range(HALVES):
                    s1[to_send(d, h) + pieces[0]] = block[:, h * CH : (h + 1) * CH].astype(bf16)
            rs_pass_b(k)
            pl.when(k == NC - 1)(lambda: pltpu.make_async_copy(a0_h, aT, sm.at[0]).start())
            wait(hid, shid.at[0])
            rs_arrived(k, 2, l2)

            @pl.when(k < NI)
            def _():
                rs_last(k)
                down = dot(dyT[...], hid[...], NT).T
                for d in range(n):
                    block = down[d * RC : (d + 1) * RC]
                    Fd[slot, d] = block
                    for h in range(HALVES):
                        for i in range(1, len(pieces)):
                            columns = down_piece(i)
                            some = block[h * SUB : (h + 1) * SUB, columns.start : columns.start + columns.size]
                            s1[to_send(d, h) + pieces[i]] = some.astype(bf16)

            rs_pass_2(k)
            rs_send(k)
            pl.when((k + 1 < NI) & (k + 1 != NC))(lambda: load_hidden(k + 1))

            @pl.when(k + 1 == NC)
            def _():
                for b in range(2):
                    each_h(b, lambda copy: copy.start())


            def into(first, last=False):
                wait_w(slot)
                da = dot(wcomb[slot].reshape(D, WIDE), big[...])
                da = da if first else daT[...] + da
                daT[...] = da.astype(bf16).astype(f32) if last else da

            pl.when(k == 0)(lambda: into(True))
            pl.when((k > 0) & (k < NC - 1))(lambda: into(False))
            pl.when(k == NC - 1)(lambda: into(False, last=True))
            return 0

        lax.fori_loop(0, NI, one, 0)

        def rest(k, _):
            rs_early(k)
            rs_arrived_a(k)
            rs_sums_a(k)
            rs_pass_b(k)
            rs_arrived(k, 1, lb)
            rs_sums_b(k)
            rs_pass_2(k)
            rs_arrived(k, 2, l2)
            rs_last(k)
            return 0

        lax.fori_loop(NI, NI + 4, rest, 0)

    pl.run_scoped(
        backward,
        vmem((D, T), f32),
        vmem((WIDE, T), bf16),
        vmem((n * RC, T), bf16),
        vmem((SLOTS, n, R, WIDE), f32),
        vmem((SLOTS, n, RC, D), f32),
        vmem((SLOTS, HALVES, S, S, RB, CH), bf16),
        vmem((SLOTS, HALVES, S, RB, CH), bf16),
        vmem((SLOTS, HALVES, S, RB, CH), bf16),
        vmem((SLOTS, HALVES, S, RB, CH), f32),
        vmem((SLOTS, HALVES, RB, CH), f32),
        vmem(rA.shape[2:], bf16),
        dma((SLOTS,)),
    )

    results = [pltpu.make_async_copy(here, to, sm.at[i]) for i, (here, to) in enumerate(((gg, gg_h), (gu, gu_h), (gd, gd_h)))]
    for copy in results:
        copy.start()
    sst[...] = acc[...]
    ssr[me] = acc[...]
    for r in range(1, n):
        send(sst, ssr.at[me], ss_s, ss_r, {"dp": (me + r) % n})
    wait(ssr.at[pl.ds(0, n - 1)], ss_r)
    wait(ssr.at[pl.ds(0, n - 1)], ss_s)
    total = ssr[0]
    for d in range(1, n):
        total += ssr[d]
    ss[...] = total
    for copy in results:
        copy.wait()


def solution(mesh):
    n = mesh.shape["dp"]
    S = math.isqrt(n)

    def step(x, dy, *arrays):
        weights, m, v = (arrays[i : i + 3] for i in (0, 3, 6))
        L, R, FF = weights[0].shape
        RF, D = weights[2].shape[1:]
        T = x.shape[1]
        NC = FF // CH
        RB = R + SUB * pl.cdiv(D, CH)
        NJ = T // TB
        sds = jax.ShapeDtypeStruct
        vmem, dma = pltpu.VMEM, pltpu.SemaphoreType.DMA
        outs = [
            (sds((L, R, FF), bf16), pl.ANY),
            (sds((L, R, FF), bf16), pl.ANY),
            (sds((L, RF, D), bf16), pl.ANY),
            (sds(TILE, f32), pltpu.VMEM),
            (sds((2, L, NC, S, S, R, CH), bf16), pl.ANY),
            (sds((L, FF, D), bf16), pl.ANY),
            (sds((L, NC, WIDE, T), f32), pl.ANY),
            (sds((L, FF, T), bf16), pl.ANY),
            (sds((D, T), bf16), pl.ANY),
            (sds((D, T), bf16), pl.ANY),
            (sds((L, NC, HALVES, HALVES, PAIR, PAIR, RB, CH), bf16), pl.ANY),
        ]
        scratch = [
            vmem((L, R, FF), bf16),
            vmem((L, R, FF), bf16),
            vmem((L, RF, D), bf16),
            vmem((SLOTS, D, T), bf16),
            vmem((NJ, WIDE, TB), f32),
            vmem((SLOTS, S, S, R, WIDE), bf16),
            vmem((SLOTS, CH, D), bf16),
            vmem((1, T), f32),
            vmem(TILE, f32),
            vmem(TILE, f32),
            vmem((n,) + TILE, f32),
            vmem((3, HALVES, HALVES, PAIR, RB, CH), bf16),
            vmem((AHEAD, HALVES, S - 1, RB, CH), bf16),
            dma((SLOTS,)),
            dma((2, 2)),
            dma((SLOTS,)),
            dma((NJ,)),
            dma((SLOTS,)),
            dma((3,)),
            dma((AHEAD, 2)),
            dma((3, AHEAD, 2)),
            dma((3, L * NC, 2)),
            dma((3, SLOTS)),
            dma((L * NC, 3)),
            dma(()),
            dma(()),
            dma(()),
        ]
        flops = 15 * 2 * T * D * FF
        done = pl.pallas_call(
            lambda *refs: step_kernel(n, *refs),
            in_specs=[pl.BlockSpec(memory_space=pl.ANY)] * 5,
            out_specs=[pl.BlockSpec(memory_space=space) for _, space in outs],
            out_shape=[shape for shape, _ in outs],
            scratch_shapes=scratch,
            compiler_params=pltpu.CompilerParams(
                collective_id=0,
                has_side_effects=True,
                vmem_limit_bytes=VMEM_BYTES,
            ),
            cost_estimate=pl.CostEstimate(flops=flops, bytes_accessed=400 << 20, transcendentals=0),
            name="train_step",
        )(x[0], dy[0], *weights)
        gradients = done[:3]
        count = n * sum(g.size for g in gradients)
        old = [array for g, w, m_, v_ in zip(gradients, weights, m, v, strict=True) for array in (g, w, m_, v_)]
        new = pl.pallas_call(
            lambda *refs: adamw_kernel(count, *refs),
            in_specs=[pl.BlockSpec(memory_space=pltpu.VMEM)] + [pl.BlockSpec(memory_space=pl.ANY)] * len(old),
            out_specs=[pl.BlockSpec(memory_space=pl.ANY)] * (len(weights) * 3),
            out_shape=[sds(a.shape, a.dtype) for w, m_, v_ in zip(weights, m, v, strict=True) for a in (w, m_, v_)],
            scratch_shapes=[vmem(a.shape, a.dtype) for a in old] + [dma((len(old),))],
            compiler_params=pltpu.CompilerParams(vmem_limit_bytes=VMEM_BYTES),
            name="adamw",
        )(done[3], *old)
        return tuple(new[i] for which in range(3) for i in range(which, len(new), 3))

    states, cut = P(("rep", "dp"), None, None), P(None, "dp", None)
    return jax.shard_map(
        step,
        mesh=mesh,
        in_specs=(states, states) + (cut,) * 9,
        out_specs=(P("rep", "dp", None),) * 9,
        check_vma=False,
    )
```
